128 devices in a mesh: gx: 4 (over z), gy: 16 (over y, x), gz: 2 (over core).
Axes of the slice: x: 4, y: 4, z: 4, core: 2. Of those that a mesh axis runs over, the one named last changes fastest.
Arguments:
- particles: float32 [8, 1048576], P(None, ('gx', 'gy', 'gz')), may hold values from -0.5 to 0.5
- dest_key: int32 [1048576], P(('gx', 'gy', 'gz')), may hold values from 0 to 127, as said below
- cell_a: int32 [1048576], P(('gx', 'gy', 'gz')), may hold values from 0 to 255
- cell_b: int32 [1048576], P(('gx', 'gy', 'gz')), may hold values from 0 to 127
- velocity: float32 [2, 1024, 4096], P(None, 'gx', ('gy', 'gz')), may hold values from -6 to 6
Outputs:
- binned: float32 [8, 4194304], P(None, ('gx', 'gy', 'gz'))
- binned_cell: int32 [4194304], P(('gx', 'gy', 'gz'))
The draws below stay inside these ranges and needn't reach their ends.
Inputs may be any that keep to these rules, and one draw needn't show every extreme that they name: Of the particles of one device at most 256 have any one value of dest_key, and one device is named by exactly 256 particles of every device.
All inputs are finite; a program needn't handle non-finite values.
Results may differ from the reference program's by a relative error of at most 0.0003.
Values sent between devices are 32-bit elements; how exact they have to be, the bound alone decides.
A program may use at most 64 MiB of HBM per device.

```python
import jax
import jax.numpy as jnp
from jax import lax

P_DEV = 8192
TA = 256
TB = 128
OWNERS = 128
CAP = 256
TOTAL = 1048576
NA = 1024
NB = 4096
N_GY = 16
N_GZ = 2


def draw_dest_key(key, part):
    hot_owner = jax.random.randint(jax.random.fold_in(key, 7), (), 0, OWNERS)
    slot_owner = (jnp.arange(OWNERS * CAP, dtype=jnp.int32) // CAP + hot_owner) % OWNERS

    def one_source(source_dev):
        source_key = jax.random.fold_in(key, source_dev)
        others = jax.random.permutation(source_key, OWNERS * CAP - CAP).astype(jnp.int32) + CAP
        chosen = jnp.concatenate([jnp.arange(CAP, dtype=jnp.int32), others[:P_DEV - CAP]])
        shuffle = jax.random.permutation(jax.random.fold_in(source_key, 1), P_DEV)
        return slot_owner[chosen][shuffle]
    return lax.map(one_source, jnp.arange(OWNERS, dtype=jnp.int32)).reshape(-1)


def place_ends(array, stream_key, smallest, top_value):
    longest = array.shape.index(max(array.shape))
    spots = []
    for shift in (0, 1):
        where = [jax.random.randint(jax.random.fold_in(stream_key, axis), (), 0, length) for axis, length in enumerate(array.shape)]
        where[longest] = (where[longest] + shift) % array.shape[longest]
        spots.append(tuple(where))
    return array.at[spots[0]].set(smallest).at[spots[1]].set(top_value)


def level_of(rng, extent, split, low, high):
    def one(dim, shards_of):
        heights = jax.random.uniform(jax.random.fold_in(jax.random.fold_in(rng, 6), dim), (shards_of,), jnp.float32, low / len(split), high / len(split))
        return jnp.repeat(jnp.exp(heights), extent[dim] // shards_of).reshape((-1,) + (1,) * (len(extent) - dim - 1))

    gain = one(*split[0])
    for cut in split[1:]:
        gain = gain * one(*cut)
    return gain


def scatter_about(key, shape, spread, limit, cuts=(), held_as=jnp.bfloat16):
    drawn = spread * jax.random.normal(key, shape, jnp.float32)
    if cuts:
        drawn = drawn * level_of(key, shape, cuts, -0.22, 0.18)
    return jnp.clip(drawn, -limit, limit).astype(held_as)


def setup_inputs(seed: int = 0) -> dict:
    splits = jax.random.split(jax.random.key(seed), 6)
    particles = jnp.clip(jax.random.uniform(splits[0], (8, TOTAL), jnp.float32, -0.5, 0.5) * level_of(splits[0], (8, TOTAL), ((1, 128),), -0.4, 0.0), -0.5, 0.5)
    dest_key = draw_dest_key(jax.random.fold_in(splits[5], 71), 0)
    cell_a = place_ends(jax.random.randint(splits[2], (TOTAL,), 0, TA), jax.random.fold_in(splits[2], 1), 0, TA - 1).astype(jnp.int32)
    cell_b = place_ends(jax.random.randint(splits[3], (TOTAL,), 0, TB), jax.random.fold_in(splits[3], 1), 0, TB - 1).astype(jnp.int32)
    velocity = scatter_about(splits[4], (2, NA, NB), 1.0, 6.0, ((1, 4), (2, 32)), jnp.float32)
    return {"particles": particles, "dest_key": dest_key, "cell_a": cell_a, "cell_b": cell_b, "velocity": velocity}


step_length = 0.5


def quad_weights(frac):
    return (0.5 * frac * (frac - 1.0), 1.0 - frac * frac, 0.5 * frac * (frac + 1.0))


def reference(particles, dest_key, cell_a, cell_b, velocity):
    source_dev = jnp.arange(TOTAL, dtype=jnp.int32) // P_DEV
    bucket_key = source_dev * OWNERS + dest_key
    ordering = jnp.argsort(bucket_key, stable=True).astype(jnp.int32)
    ordered = bucket_key[ordering]
    first_index = jnp.searchsorted(ordered, ordered, side="left").astype(jnp.int32)
    rank_sorted = jnp.arange(TOTAL, dtype=jnp.int32) - first_index
    ranking = jnp.zeros((TOTAL,), jnp.int32).at[ordering].set(rank_sorted)
    slot_index = dest_key * (OWNERS * CAP) + source_dev * CAP + ranking
    tile_columns = N_GY * N_GZ
    global_a = (dest_key // tile_columns) * TA + cell_a
    global_b = (dest_key % tile_columns) * TB + cell_b
    padded = jnp.pad(velocity, ((0, 0), (1, 1), (1, 1)))
    row_stride = NB + 2
    flat_field = padded.reshape(2, -1)
    center = ((global_a + 1) * row_stride + global_b + 1).astype(jnp.int32)
    weights_a = quad_weights(particles[0])
    weights_b = quad_weights(particles[1])
    speed = jnp.zeros((2, TOTAL), jnp.float32)
    for shift_a in range(3):
        for shift_b in range(3):
            nodes = flat_field[:, center + (shift_a - 1) * row_stride + (shift_b - 1)]
            speed = speed + weights_a[shift_a] * weights_b[shift_b] * nodes
    advanced = jnp.concatenate([particles[0:2], particles[2:4] + step_length * speed, particles[4:8]], axis=0)
    binned = jnp.zeros((8, OWNERS * OWNERS * CAP), particles.dtype).at[:, slot_index].set(advanced)
    binned_cell = jnp.full((OWNERS * OWNERS * CAP,), -1, jnp.int32).at[slot_index].set(cell_a * TB + cell_b)
    return binned, binned_cell
```

```python
import functools

import jax
import jax.numpy as jnp
from jax import lax
from jax.experimental import pallas as pl
from jax.experimental.pallas import tpu as pltpu
from jax.sharding import PartitionSpec as P

AXES = ("gx", "gy", "gz")
MESH = pl.DeviceIdType.MESH
F32, BF16, I32 = jnp.float32, jnp.bfloat16, jnp.int32
CAP = 256
CHUNK = 1024
LANES = 128
step_length = 0.5


def quad_weights(frac):
    return (0.5 * frac * (frac - 1.0), 1.0 - frac * frac, 0.5 * frac * (frac + 1.0))


def two_parts(x):
    high = x.astype(BF16)
    return high, (x - high.astype(F32)).astype(BF16)


def sort_kernel(
    part_ref, key_ref, a_ref, b_ref, vel_ref, out_ref, cell_ref, turned_ref,
    pos_ref, acc_ref, sorted_ref, sorted_cell_ref, table_ref, table_smem, sem,
):
    count = part_ref.shape[1]
    owners = out_ref.shape[0]
    chunks = count // CHUNK
    turned_ref[0] = vel_ref[0].T
    turned_ref[1] = vel_ref[1].T

    owner_ids = lax.broadcasted_iota(I32, (owners, CHUNK), 0)

    def count_chunk(i, total):
        keys = key_ref[:, pl.ds(pl.multiple_of(i * CHUNK, CHUNK), CHUNK)]
        hot = (owner_ids == keys).astype(F32)
        for j in range(CHUNK // LANES):
            total = total + hot[:, j * LANES : (j + 1) * LANES]
        return total

    spread = lax.fori_loop(0, chunks, count_chunk, jnp.zeros((owners, LANES), F32))
    hist = jnp.broadcast_to(jnp.sum(spread, axis=1, keepdims=True), (owners, owners))
    row = lax.broadcasted_iota(I32, (owners, owners), 0)
    col = lax.broadcasted_iota(I32, (owners, owners), 1)
    below = (col < row).astype(F32).astype(BF16)
    starts = jnp.dot(below, hist.astype(BF16), preferred_element_type=F32)
    table_ref[0:8, :] = starts.T[0:8, :].astype(I32)
    table_ref[8:16, :] = hist.T[0:8, :].astype(I32)
    copy = pltpu.make_async_copy(table_ref, table_smem, sem)
    copy.start()

    upper = (
        lax.broadcasted_iota(I32, (CAP, CAP), 0) <= lax.broadcasted_iota(I32, (CAP, CAP), 1)
    ).astype(F32).astype(BF16)
    block_ids = lax.broadcasted_iota(I32, (owners, CAP), 0)

    def rank_chunk(i, base):
        for j in range(CHUNK // CAP):
            at = pl.ds(pl.multiple_of(i * CHUNK + j * CAP, CAP), CAP)
            hot = (block_ids == key_ref[:, at]).astype(F32)
            upto = jnp.dot(hot.astype(BF16), upper, preferred_element_type=F32)
            places = jnp.sum(hot * (upto + base), axis=0, keepdims=True) - 1.0
            pos_ref[:, at] = places.astype(I32)
            base = base + upto[:, CAP - 1 : CAP]
        return base

    lax.fori_loop(0, chunks, rank_chunk, starts[:, 0:1])

    acc_ref[...] = jnp.zeros_like(acc_ref)
    lane_ids = lax.broadcasted_iota(I32, (CAP, CHUNK), 0)
    page_ids = lax.broadcasted_iota(I32, (32, CHUNK), 0)

    def place_chunk(i, carry):
        at = pl.ds(pl.multiple_of(i * CHUNK, CHUNK), CHUNK)
        pos = pos_ref[:, at]
        page = pos >> 8
        lane_hot = (lane_ids == (pos & 255)).astype(F32).astype(BF16)
        values = jnp.concatenate(two_parts(part_ref[:, at]), axis=0)
        page16 = jnp.broadcast_to(page, (16, CHUNK)).astype(F32).astype(BF16)
        zero = jnp.zeros((16, CHUNK), BF16)
        rows = [jnp.where(page16 == BF16(h), values, zero) for h in range(32)]
        page_hot = (page_ids == page)
        rows.append(jnp.where(page_hot, a_ref[:, at].astype(F32), 0.0).astype(BF16))
        rows.append(jnp.where(page_hot, b_ref[:, at].astype(F32), 0.0).astype(BF16))
        acc_ref[...] += lax.dot_general(
            jnp.concatenate(rows, axis=0), lane_hot, (((1,), (1,)), ((), ())),
            preferred_element_type=F32,
        )
        return carry

    lax.fori_loop(0, chunks, place_chunk, 0)

    cells = (acc_ref[512:544, :] * 128.0 + acc_ref[544:576, :]).astype(I32)
    for h in range(32):
        both = acc_ref[16 * h : 16 * h + 8, :] + acc_ref[16 * h + 8 : 16 * h + 16, :]
        for j in range(2):
            sorted_ref[2 * h + j] = both[:, j * LANES : (j + 1) * LANES]
            sorted_cell_ref[2 * h + j] = cells[h : h + 1, j * LANES : (j + 1) * LANES]
    for j in range(64, 67):
        sorted_ref[j] = jnp.zeros((8, LANES), F32)
        sorted_cell_ref[j] = jnp.zeros((1, LANES), I32)
    copy.wait()

    lanes8 = lax.broadcasted_iota(I32, (8, LANES), 1)
    lanes1 = lax.broadcasted_iota(I32, (1, LANES), 1)

    def expand(d, carry):
        start = table_smem[0, d]
        live = table_smem[8, d]
        page = start >> 7
        shift = start & 127
        turn = (LANES - shift) & 127
        head8, head1 = lanes8 < LANES - shift, lanes1 < LANES - shift
        rolled = [pltpu.roll(sorted_ref[page + j], turn, 1) for j in range(3)]
        cell_rolled = [pltpu.roll(sorted_cell_ref[page + j], turn, 1) for j in range(3)]
        for j in range(2):
            here = slice(j * LANES, (j + 1) * LANES)
            value = jnp.where(head8, rolled[j], rolled[j + 1])
            out_ref[d, :, here] = jnp.where(lanes8 < live - j * LANES, value, 0.0)
            cell = jnp.where(head1, cell_rolled[j], cell_rolled[j + 1])
            cell_ref[d, :, here] = jnp.where(lanes1 < live - j * LANES, cell, -1)
        return carry

    lax.fori_loop(0, owners, expand, 0, unroll=8)


def sorted_blocks(particles, dest_key, cell_a, cell_b, velocity, owners):
    count = particles.shape[1]
    tile = velocity.shape
    vmem = pl.BlockSpec(memory_space=pltpu.VMEM)
    return pl.pallas_call(
        sort_kernel,
        out_shape=(
            jax.ShapeDtypeStruct((owners, 8, CAP), F32),
            jax.ShapeDtypeStruct((owners, 1, CAP), I32),
            jax.ShapeDtypeStruct((tile[0], tile[2], tile[1]), F32),
        ),
        in_specs=[vmem] * 5,
        out_specs=(vmem,) * 3,
        scratch_shapes=[
            pltpu.VMEM((1, count), I32),
            pltpu.VMEM((576, CAP), F32),
            pltpu.VMEM((67, 8, LANES), F32),
            pltpu.VMEM((67, 1, LANES), I32),
            pltpu.VMEM((16, LANES), I32),
            pltpu.SMEM((16, LANES), I32),
            pltpu.SemaphoreType.DMA,
        ],
        name="sort",
    )(particles, dest_key.reshape(1, -1), cell_a.reshape(1, -1), cell_b.reshape(1, -1), velocity)


def exchange_kernel(
    sizes, out_ref, cell_ref, vel_ref, turned_ref,
    in_ref, in_cell_ref, rows_ref, cols_ref,
    send_sem, recv_sem, cell_send, cell_recv, halo_send, halo_recv, own_sem,
):
    nx, ny, nz = sizes
    total = nx * ny * nz
    x, y, z = (lax.axis_index(a) for a in AXES)
    me = (x * ny + y) * nz + z

    own = pltpu.make_async_copy(out_ref.at[me], in_ref.at[me], own_sem.at[0])
    own_cell = pltpu.make_async_copy(cell_ref.at[me], in_cell_ref.at[me], own_sem.at[1])
    own.start()
    own_cell.start()

    tiles = ny * nz
    tile = y * nz + z
    height = vel_ref.shape[1]
    width = vel_ref.shape[2]
    halos = []
    n = 0
    for i, dx in enumerate((1, -1)):
        to_x = lax.rem(x + dx + nx, nx)
        edge = vel_ref.at[:, pl.ds(height - 8 if dx == 1 else 0, 8), :]
        for j, dt in enumerate((1, 0, -1)):
            to_t = lax.rem(tile + dt + tiles, tiles)
            halos.append((edge, rows_ref.at[3 * i + j], to_x, to_t, n))
            n += 1
    for i, dt in enumerate((1, -1)):
        edge = turned_ref.at[:, pl.ds(width - 8 if dt == 1 else 0, 8), :]
        to_t = lax.rem(tile + dt + tiles, tiles)
        halos.append((edge, cols_ref.at[i], x, to_t, n))
        n += 1
    halo_copies = [
        pltpu.make_async_remote_copy(
            src_ref=src, dst_ref=dst, send_sem=halo_send.at[k], recv_sem=halo_recv.at[k],
            device_id=(to_x, to_t // nz, lax.rem(to_t, nz)), device_id_type=MESH,
        )
        for src, dst, to_x, to_t, k in halos
    ]
    for c in halo_copies:
        c.start()

    def send(k, carry):
        dx, dy, dz = k // (ny * nz), lax.rem(k // nz, ny), lax.rem(k, nz)
        to_x = lax.rem(x + dx, nx)
        to_yy = lax.rem(y // 4 + dy // 4, ny // 4)
        to_yx = lax.rem(lax.rem(y, 4) + lax.rem(dy, 4), 4)
        to_y = to_yy * 4 + to_yx
        to_z = lax.rem(z + dz, nz)
        there = (to_x * ny + to_y) * nz + to_z
        device = (to_x, to_y, to_z)
        pltpu.make_async_remote_copy(
            src_ref=out_ref.at[there], dst_ref=in_ref.at[me], send_sem=send_sem, recv_sem=recv_sem,
            device_id=device, device_id_type=MESH,
        ).start()
        pltpu.make_async_remote_copy(
            src_ref=cell_ref.at[there], dst_ref=in_cell_ref.at[me], send_sem=cell_send, recv_sem=cell_recv,
            device_id=device, device_id_type=MESH,
        ).start()
        return carry

    lax.fori_loop(1, total, send, 0)
    some, some_cell = in_ref.at[pl.ds(0, total - 1)], in_cell_ref.at[pl.ds(0, total - 1)]
    own.wait()
    own_cell.wait()
    for c in halo_copies:
        c.wait()
    pltpu.make_async_copy(some, some, recv_sem).wait()
    pltpu.make_async_copy(some_cell, some_cell, cell_recv).wait()
    pltpu.make_async_copy(some, some, send_sem).wait()
    pltpu.make_async_copy(some_cell, some_cell, cell_send).wait()


def exchanged(blocks, cells, velocity, turned, sizes):
    parts, height, width = velocity.shape
    vmem = pl.BlockSpec(memory_space=pltpu.VMEM)
    dma = pltpu.SemaphoreType.DMA
    return pl.pallas_call(
        functools.partial(exchange_kernel, sizes),
        out_shape=(
            jax.ShapeDtypeStruct(blocks.shape, F32),
            jax.ShapeDtypeStruct(cells.shape, I32),
            jax.ShapeDtypeStruct((6, parts, 8, width), F32),
            jax.ShapeDtypeStruct((2, parts, 8, height), F32),
        ),
        in_specs=[vmem] * 4,
        out_specs=(vmem,) * 4,
        scratch_shapes=[dma, dma, dma, dma, dma((8,)), dma((8,)), dma((2,))],
        compiler_params=pltpu.CompilerParams(has_side_effects=True),
        name="exchange",
    )(blocks, cells, velocity, turned)


def interpolate_kernel(
    sizes, in_ref, cell_ref, turned_ref, rows_ref, cols_ref, out_ref, out_cell_ref,
    high_ref, low_ref, up_ref, down_ref,
):
    nx, ny, nz = sizes
    width, height = turned_ref.shape[1], turned_ref.shape[2]
    group = in_ref.shape[0]

    @pl.when(pl.program_id(0) == 0)
    def prepare():
        x = lax.axis_index("gx")
        tile = lax.axis_index("gy") * nz + lax.axis_index("gz")
        has_left, has_right = tile > 0, tile < ny * nz - 1
        left = [jnp.where(has_left, cols_ref[0, c, 7:8, :], 0.0) for c in range(2)]
        right = [jnp.where(has_right, cols_ref[1, c, 0:1, :], 0.0) for c in range(2)]
        zeros = jnp.zeros((4, height), F32)
        sides = jnp.concatenate([left[0], right[0], left[1], right[1], zeros], axis=0)
        for c, at in ((0, 0), (1, width), (None, 2 * width)):
            block = sides if c is None else turned_ref[c]
            high, low = two_parts(block)
            high_ref[at : at + block.shape[0], :] = high
            low_ref[at : at + block.shape[0], :] = low
        for ref, first, row, there in ((up_ref, 0, 7, x > 0), (down_ref, 3, 0, x < nx - 1)):
            corner = []
            for c in range(2):
                line = jnp.where(there, rows_ref[first + 1, c], 0.0).T[:, row : row + 1]
                ref[c * width : (c + 1) * width, :] = jnp.broadcast_to(line, (width, LANES))
                from_left = rows_ref[first, c][row : row + 1, width - 1 : width]
                from_right = rows_ref[first + 2, c][row : row + 1, 0:1]
                corner.append(jnp.where(there & has_left, from_left, 0.0))
                corner.append(jnp.where(there & has_right, from_right, 0.0))
            ref[2 * width :, :] = jnp.broadcast_to(
                jnp.concatenate(corner + [jnp.zeros((4, 1), F32)], axis=0), (8, LANES)
            )

    row_ids = lax.broadcasted_iota(I32, (height, CAP), 0).astype(F32).astype(BF16)
    col_ids = lax.broadcasted_iota(I32, (width, CAP), 0)
    sub_ids = lax.broadcasted_iota(I32, (8, CAP), 0)

    def one_source(s, carry):
        data = in_ref[s]
        cell = cell_ref[s]
        live = cell >= 0
        node_a = jnp.where(live, cell >> 7, 2 * height)
        node_b = cell & 127
        below, same, above = quad_weights(data[0:1, :])
        left, mid, right = quad_weights(data[1:2, :])
        a16 = node_a.astype(F32).astype(BF16)
        is_same = row_ids == a16
        is_below = row_ids == a16 - BF16(1)
        is_above = row_ids == a16 + BF16(1)
        weights = []
        for part in zip(two_parts(below), two_parts(same), two_parts(above)):
            weights.append(
                jnp.where(is_below, part[0], jnp.where(is_same, part[1], jnp.where(is_above, part[2], BF16(0))))
            )
        dot = functools.partial(jnp.dot, preferred_element_type=F32)
        mixed = dot(high_ref[...], weights[0]) + dot(high_ref[...], weights[1]) + dot(low_ref[...], weights[0])
        first = node_a == 0
        edge = jnp.where(first, below, jnp.where(node_a == height - 1, above, 0.0))
        up = jnp.concatenate([up_ref[...]] * 2, axis=1)
        down = jnp.concatenate([down_ref[...]] * 2, axis=1)
        mixed = mixed + jnp.where(first, up, down) * edge
        cols = jnp.where(
            col_ids == node_b - 1, left, jnp.where(col_ids == node_b, mid, jnp.where(col_ids == node_b + 1, right, 0.0))
        )
        at_left = jnp.where(node_b == 0, left, 0.0)
        at_right = jnp.where(node_b == width - 1, right, 0.0)
        speed = []
        for c in range(2):
            inner = jnp.sum(mixed[c * width : (c + 1) * width, :] * cols, axis=0, keepdims=True)
            side = 2 * width + 2 * c
            speed.append(
                inner + mixed[side : side + 1, :] * at_left + mixed[side + 1 : side + 2, :] * at_right
            )
        shift = jnp.where(sub_ids == 2, speed[0], jnp.where(sub_ids == 3, speed[1], 0.0))
        here = pl.ds(pl.multiple_of(s * CAP, CAP), CAP)
        out_ref[:, here] = data + step_length * shift
        out_cell_ref[s] = cell
        return carry

    lax.fori_loop(0, group, one_source, 0, unroll=2)


def interpolated(blocks, cells, turned, rows, cols, sizes):
    sources = blocks.shape[0]
    parts, width, height = turned.shape
    group = 8
    whole = pl.BlockSpec(memory_space=pltpu.VMEM)
    return pl.pallas_call(
        functools.partial(interpolate_kernel, sizes),
        grid=(sources // group,),
        out_shape=(
            jax.ShapeDtypeStruct((8, sources * CAP), F32),
            jax.ShapeDtypeStruct((sources, 1, CAP), I32),
        ),
        in_specs=[
            pl.BlockSpec((group, 8, CAP), lambda i: (i, 0, 0)),
            pl.BlockSpec((group, 1, CAP), lambda i: (i, 0, 0)),
            whole, whole, whole,
        ],
        out_specs=(
            pl.BlockSpec((8, group * CAP), lambda i: (0, i)),
            pl.BlockSpec((group, 1, CAP), lambda i: (i, 0, 0)),
        ),
        scratch_shapes=[
            pltpu.VMEM((2 * width + 8, height), BF16),
            pltpu.VMEM((2 * width + 8, height), BF16),
            pltpu.VMEM((2 * width + 8, LANES), F32),
            pltpu.VMEM((2 * width + 8, LANES), F32),
        ],
        name="interpolate",
    )(blocks, cells, turned, rows, cols)


def shards(sizes, particles, dest_key, cell_a, cell_b, velocity):
    owners = sizes[0] * sizes[1] * sizes[2]
    blocks, cells, turned = sorted_blocks(particles, dest_key, cell_a, cell_b, velocity, owners)
    arrived, arrived_cells, rows, cols = exchanged(blocks, cells, velocity, turned, sizes)
    binned, binned_cell = interpolated(arrived, arrived_cells, turned, rows, cols, sizes)
    return binned, binned_cell.reshape(-1)


def solution(mesh):
    sizes = tuple(mesh.shape[a] for a in AXES)
    in_specs = (P(None, AXES), P(AXES), P(AXES), P(AXES), P(None, "gx", ("gy", "gz")))
    out_specs = (P(None, AXES), P(AXES))
    return jax.shard_map(
        functools.partial(shards, sizes), mesh=mesh, in_specs=in_specs, out_specs=out_specs, check_vma=False
    )
```

```python
import functools

import jax
import jax.numpy as jnp
from jax import lax
from jax.experimental import pallas as pl
from jax.experimental.pallas import tpu as pltpu
from jax.sharding import PartitionSpec as P

AXES = ("gx", "gy", "gz")
MESH = pl.DeviceIdType.MESH
F32, BF16, I32 = jnp.float32, jnp.bfloat16, jnp.int32
CAP = 256
CHUNK = 1024
LANES = 128
step_length = 0.5


def quad_weights(frac):
    return (0.5 * frac * (frac - 1.0), 1.0 - frac * frac, 0.5 * frac * (frac + 1.0))


def two_parts(x):
    high = x.astype(BF16)
    return high, (x - high.astype(F32)).astype(BF16)


def sort_phase(
    part_ref, key_ref, a_ref, b_ref,
    pos_ref, acc_ref, sorted_ref, sorted_cell_ref, table_ref, table_smem, sem, owners, between,
):
    count = part_ref.shape[1]
    chunks = count // CHUNK

    owner_ids = lax.broadcasted_iota(I32, (owners, CHUNK), 0)

    def count_chunk(i, total):
        keys = key_ref[:, pl.ds(pl.multiple_of(i * CHUNK, CHUNK), CHUNK)]
        hot = (owner_ids == keys).astype(F32)
        for j in range(CHUNK // LANES):
            total = total + hot[:, j * LANES : (j + 1) * LANES]
        return total

    spread = lax.fori_loop(0, chunks, count_chunk, jnp.zeros((owners, LANES), F32))
    hist = jnp.broadcast_to(jnp.sum(spread, axis=1, keepdims=True), (owners, owners))
    row = lax.broadcasted_iota(I32, (owners, owners), 0)
    col = lax.broadcasted_iota(I32, (owners, owners), 1)
    below = (col < row).astype(F32).astype(BF16)
    starts = jnp.dot(below, hist.astype(BF16), preferred_element_type=F32)
    table_ref[0:8, :] = starts.T[0:8, :].astype(I32)
    table_ref[8:16, :] = hist.T[0:8, :].astype(I32)
    copy = pltpu.make_async_copy(table_ref, table_smem, sem)
    copy.start()

    upper = (
        lax.broadcasted_iota(I32, (CAP, CAP), 0) <= lax.broadcasted_iota(I32, (CAP, CAP), 1)
    ).astype(F32).astype(BF16)
    block_ids = lax.broadcasted_iota(I32, (owners, CAP), 0)

    def rank_chunk(i, base):
        for j in range(CHUNK // CAP):
            at = pl.ds(pl.multiple_of(i * CHUNK + j * CAP, CAP), CAP)
            hot = (block_ids == key_ref[:, at]).astype(F32)
            upto = jnp.dot(hot.astype(BF16), upper, preferred_element_type=F32)
            places = jnp.sum(hot * (upto + base), axis=0, keepdims=True) - 1.0
            pos_ref[:, at] = places.astype(I32)
            base = base + upto[:, CAP - 1 : CAP]
        return base

    lax.fori_loop(0, chunks, rank_chunk, starts[:, 0:1])
    between()

    acc_ref[...] = jnp.zeros_like(acc_ref)
    lane_ids = lax.broadcasted_iota(I32, (CAP, CHUNK), 0)
    page_ids = lax.broadcasted_iota(I32, (32, CHUNK), 0)

    def place_chunk(i, carry):
        at = pl.ds(pl.multiple_of(i * CHUNK, CHUNK), CHUNK)
        pos = pos_ref[:, at]
        page = pos >> 8
        lane_hot = (lane_ids == (pos & 255)).astype(F32).astype(BF16)
        values = jnp.concatenate(two_parts(part_ref[:, at]), axis=0)
        page16 = jnp.broadcast_to(page, (16, CHUNK)).astype(F32).astype(BF16)
        zero = jnp.zeros((16, CHUNK), BF16)
        rows = [jnp.where(page16 == BF16(h), values, zero) for h in range(32)]
        page_hot = (page_ids == page)
        rows.append(jnp.where(page_hot, a_ref[:, at].astype(F32), 0.0).astype(BF16))
        rows.append(jnp.where(page_hot, b_ref[:, at].astype(F32), 0.0).astype(BF16))
        acc_ref[...] += lax.dot_general(
            jnp.concatenate(rows, axis=0), lane_hot, (((1,), (1,)), ((), ())),
            preferred_element_type=F32,
        )
        return carry

    lax.fori_loop(0, chunks, place_chunk, 0)

    cells = (acc_ref[512:544, :] * 128.0 + acc_ref[544:576, :]).astype(I32)
    for h in range(32):
        both = acc_ref[16 * h : 16 * h + 8, :] + acc_ref[16 * h + 8 : 16 * h + 16, :]
        for j in range(2):
            sorted_ref[2 * h + j] = both[:, j * LANES : (j + 1) * LANES]
            sorted_cell_ref[2 * h + j] = cells[h : h + 1, j * LANES : (j + 1) * LANES]
    for j in range(64, 67):
        sorted_ref[j] = jnp.zeros((8, LANES), F32)
        sorted_cell_ref[j] = jnp.zeros((1, LANES), I32)
    copy.wait()


def expand(d, sorted_ref, sorted_cell_ref, table_smem, send_ref, send_cell_ref):
    lanes8 = lax.broadcasted_iota(I32, (8, LANES), 1)
    lanes1 = lax.broadcasted_iota(I32, (1, LANES), 1)
    start = jnp.clip(table_smem[0, d], 0, LANES * (sorted_ref.shape[0] - 3))
    live = table_smem[8, d]
    page = start >> 7
    shift = start & 127
    turn = (LANES - shift) & 127
    head8, head1 = lanes8 < LANES - shift, lanes1 < LANES - shift
    rolled = [pltpu.roll(sorted_ref[page + j], turn, 1) for j in range(3)]
    cell_rolled = [pltpu.roll(sorted_cell_ref[page + j], turn, 1) for j in range(3)]
    for j in range(2):
        here = slice(j * LANES, (j + 1) * LANES)
        value = jnp.where(head8, rolled[j], rolled[j + 1])
        send_ref[d, :, here] = jnp.where(lanes8 < live - j * LANES, value, 0.0)
        cell = jnp.where(head1, cell_rolled[j], cell_rolled[j + 1])
        send_cell_ref[d, :, here] = jnp.where(lanes1 < live - j * LANES, cell, -1)


def prepare_field(sizes, turned_ref, rows_ref, cols_ref, high_ref, low_ref, up_ref, down_ref):
    nx, ny, nz = sizes
    width, height = turned_ref.shape[1], turned_ref.shape[2]
    x = lax.axis_index("gx")
    tile = lax.axis_index("gy") * nz + lax.axis_index("gz")
    has_left, has_right = tile > 0, tile < ny * nz - 1
    left = [jnp.where(has_left, cols_ref[0, c, 7:8, :], 0.0) for c in range(2)]
    right = [jnp.where(has_right, cols_ref[1, c, 0:1, :], 0.0) for c in range(2)]
    zeros = jnp.zeros((4, height), F32)
    sides = jnp.concatenate([left[0], right[0], left[1], right[1], zeros], axis=0)
    for c, at in ((0, 0), (1, width), (None, 2 * width)):
        block = sides if c is None else turned_ref[c]
        high, low = two_parts(block)
        high_ref[at : at + block.shape[0], :] = high
        low_ref[at : at + block.shape[0], :] = low
    for ref, first, row, there in ((up_ref, 0, 7, x > 0), (down_ref, 3, 0, x < nx - 1)):
        corner = []
        for c in range(2):
            line = jnp.where(there, rows_ref[first + 1, c], 0.0).T[:, row : row + 1]
            ref[c * width : (c + 1) * width, :] = jnp.broadcast_to(line, (width, LANES))
            from_left = rows_ref[first, c][row : row + 1, width - 1 : width]
            from_right = rows_ref[first + 2, c][row : row + 1, 0:1]
            corner.append(jnp.where(there & has_left, from_left, 0.0))
            corner.append(jnp.where(there & has_right, from_right, 0.0))
        ref[2 * width :, :] = jnp.broadcast_to(
            jnp.concatenate(corner + [jnp.zeros((4, 1), F32)], axis=0), (8, LANES)
        )


def interpolate_source(s, out_ref, cell_ref, high_ref, low_ref, up_ref, down_ref):
    height = high_ref.shape[1]
    width = (high_ref.shape[0] - 8) // 2
    row_ids = lax.broadcasted_iota(I32, (height, CAP), 0).astype(F32).astype(BF16)
    col_ids = lax.broadcasted_iota(I32, (width, CAP), 0)
    sub_ids = lax.broadcasted_iota(I32, (8, CAP), 0)
    here = pl.ds(pl.multiple_of(s * CAP, CAP), CAP)
    data = out_ref[:, here]
    cell = cell_ref[s]
    live = cell >= 0
    node_a = jnp.where(live, cell >> 7, 2 * height)
    node_b = cell & 127
    below, same, above = quad_weights(data[0:1, :])
    left, mid, right = quad_weights(data[1:2, :])
    a16 = node_a.astype(F32).astype(BF16)
    is_same = row_ids == a16
    is_below = row_ids == a16 - BF16(1)
    is_above = row_ids == a16 + BF16(1)
    weights = []
    for part in zip(two_parts(below), two_parts(same), two_parts(above)):
        weights.append(
            jnp.where(is_below, part[0], jnp.where(is_same, part[1], jnp.where(is_above, part[2], BF16(0))))
        )
    dot = functools.partial(jnp.dot, preferred_element_type=F32)
    mixed = dot(high_ref[...], weights[0]) + dot(high_ref[...], weights[1]) + dot(low_ref[...], weights[0])
    first = node_a == 0
    edge = jnp.where(first, below, jnp.where(node_a == height - 1, above, 0.0))
    up = jnp.concatenate([up_ref[...]] * 2, axis=1)
    down = jnp.concatenate([down_ref[...]] * 2, axis=1)
    mixed = mixed + jnp.where(first, up, down) * edge
    cols = jnp.where(
        col_ids == node_b - 1, left, jnp.where(col_ids == node_b, mid, jnp.where(col_ids == node_b + 1, right, 0.0))
    )
    at_left = jnp.where(node_b == 0, left, 0.0)
    at_right = jnp.where(node_b == width - 1, right, 0.0)
    speed = []
    for c in range(2):
        inner = jnp.sum(mixed[c * width : (c + 1) * width, :] * cols, axis=0, keepdims=True)
        side = 2 * width + 2 * c
        speed.append(
            inner + mixed[side : side + 1, :] * at_left + mixed[side + 1 : side + 2, :] * at_right
        )
    shift = jnp.where(sub_ids == 2, speed[0], jnp.where(sub_ids == 3, speed[1], 0.0))
    out_ref[:, here] = data + step_length * shift


GROUP = 8


def rebin_kernel(
    sizes, part_ref, key_ref, a_ref, b_ref, vel_ref, out_ref, cell_ref,
    pos_ref, acc_ref, sorted_ref, sorted_cell_ref, table_ref, table_smem,
    send_ref, send_cell_ref, turned_ref, rows_ref, cols_ref, high_ref, low_ref, up_ref, down_ref,
    table_sem, send_sem, send_cell_sem, recv_sem, recv_cell_sem, halo_send, halo_recv,
):
    nx, ny, nz = sizes
    total = nx * ny * nz
    side = 4
    x, y, z = (lax.axis_index(a) for a in AXES)
    me = (x * ny + y) * nz + z
    tiles = ny * nz
    tile = y * nz + z
    height, width = vel_ref.shape[1], vel_ref.shape[2]

    def peer(k, sign):
        dx = lax.rem(k // tiles + nx // 2, nx)
        dy = lax.rem(k // (side * nz) + ny // side // 2, ny // side)
        dyx = lax.rem(k // nz + side // 2, side)
        dz = lax.rem(k, nz)
        if sign < 0:
            dx, dy, dyx, dz = nx - dx, ny // side - dy, side - dyx, nz - dz
        to_x = lax.rem(x + dx, nx)
        to_y = lax.rem(y // side + dy, ny // side) * side + lax.rem(lax.rem(y, side) + dyx, side)
        to_z = lax.rem(z + dz, nz)
        return (to_x * ny + to_y) * nz + to_z, (to_x, to_y, to_z)

    own = ((nx // 2) * (ny // side) + ny // side // 2) * side * nz + (side // 2) * nz

    barrier = pltpu.get_barrier_semaphore()

    def greet(k, carry):
        @pl.when(k != own)
        def tell():
            pl.semaphore_signal(barrier, inc=1, device_id=peer(k, 1)[1], device_id_type=MESH)
        return carry

    lax.fori_loop(0, total, greet, 0)
    turned_ref[0] = vel_ref[0].T
    turned_ref[1] = vel_ref[1].T

    halos = []
    for i, dx in enumerate((1, -1)):
        to_x = lax.rem(x + dx + nx, nx)
        edge = vel_ref.at[:, pl.ds(height - 8 if dx == 1 else 0, 8), :]
        for j, dt in enumerate((1, 0, -1)):
            halos.append((edge, rows_ref.at[3 * i + j], to_x, lax.rem(tile + dt + tiles, tiles)))
    for i, dt in enumerate((1, -1)):
        edge = turned_ref.at[:, pl.ds(width - 8 if dt == 1 else 0, 8), :]
        halos.append((edge, cols_ref.at[i], x, lax.rem(tile + dt + tiles, tiles)))
    halo_copies = [
        pltpu.make_async_remote_copy(
            src_ref=src, dst_ref=dst, send_sem=halo_send.at[k], recv_sem=halo_recv.at[k],
            device_id=(to_x, to_t // nz, lax.rem(to_t, nz)), device_id_type=MESH,
        )
        for k, (src, dst, to_x, to_t) in enumerate(halos)
    ]

    def between():
        pl.semaphore_wait(barrier, total - 1)
        for c in halo_copies:
            c.start()

    sort_phase(
        part_ref, key_ref, a_ref, b_ref, pos_ref, acc_ref, sorted_ref, sorted_cell_ref,
        table_ref, table_smem, table_sem, total, between,
    )

    mine = pl.ds(pl.multiple_of(me * CAP, CAP), CAP)

    def send_group(g):
        def send(i, carry):
            k = g * GROUP + i
            there, device = peer(k, 1)

            @pl.when(k != own)
            def remote():
                pltpu.make_async_remote_copy(
                    src_ref=send_ref.at[there], dst_ref=out_ref.at[:, mine], send_sem=send_sem,
                    recv_sem=recv_sem.at[g], device_id=device, device_id_type=MESH,
                ).start()
                pltpu.make_async_remote_copy(
                    src_ref=send_cell_ref.at[there], dst_ref=cell_ref.at[me], send_sem=send_cell_sem,
                    recv_sem=recv_cell_sem.at[g], device_id=device, device_id_type=MESH,
                ).start()

            @pl.when(k == own)
            def local():
                pltpu.make_async_copy(send_ref.at[there], out_ref.at[:, mine], recv_sem.at[g]).start()
                pltpu.make_async_copy(send_cell_ref.at[there], cell_ref.at[me], recv_cell_sem.at[g]).start()

            return carry

        lax.fori_loop(0, GROUP, send, 0)

    def expand_group(g, carry):
        for i in range(GROUP):
            there = peer(g * GROUP + i, 1)[0]
            expand(there, sorted_ref, sorted_cell_ref, table_smem, send_ref, send_cell_ref)

        @pl.when(g > 0)
        def before():
            send_group(g - 1)

        return carry

    groups = total // GROUP
    lax.fori_loop(0, groups, expand_group, 0)
    send_group(groups - 1)

    for c in halo_copies:
        c.wait()
    prepare_field(sizes, turned_ref, rows_ref, cols_ref, high_ref, low_ref, up_ref, down_ref)

    def finish_group(g, carry):
        blocks = out_ref.at[:, pl.ds(0, GROUP * CAP)]
        pltpu.make_async_copy(blocks, blocks, recv_sem.at[g]).wait()
        few = cell_ref.at[pl.ds(0, GROUP)]
        pltpu.make_async_copy(few, few, recv_cell_sem.at[g]).wait()

        def one(i, inner):
            source = peer(g * GROUP + i, -1)[0]
            interpolate_source(source, out_ref, cell_ref, high_ref, low_ref, up_ref, down_ref)
            return inner

        lax.fori_loop(0, GROUP, one, 0, unroll=2)
        return carry

    lax.fori_loop(0, groups, finish_group, 0)
    some = send_ref.at[pl.ds(0, total - 1)]
    some_cell = send_cell_ref.at[pl.ds(0, total - 1)]
    pltpu.make_async_copy(some, some, send_sem).wait()
    pltpu.make_async_copy(some_cell, some_cell, send_cell_sem).wait()


def shards(sizes, particles, dest_key, cell_a, cell_b, velocity):
    owners = sizes[0] * sizes[1] * sizes[2]
    count = particles.shape[1]
    parts, height, width = velocity.shape
    vmem = pl.BlockSpec(memory_space=pltpu.VMEM)
    dma = pltpu.SemaphoreType.DMA
    groups = owners // GROUP
    binned, binned_cell = pl.pallas_call(
        functools.partial(rebin_kernel, sizes),
        out_shape=(
            jax.ShapeDtypeStruct((8, owners * CAP), F32),
            jax.ShapeDtypeStruct((owners, 1, CAP), I32),
        ),
        in_specs=[vmem] * 5,
        out_specs=(vmem,) * 2,
        scratch_shapes=[
            pltpu.VMEM((1, count), I32),
            pltpu.VMEM((576, CAP), F32),
            pltpu.VMEM((67, 8, LANES), F32),
            pltpu.VMEM((67, 1, LANES), I32),
            pltpu.VMEM((16, LANES), I32),
            pltpu.SMEM((16, LANES), I32),
            pltpu.VMEM((owners, 8, CAP), F32),
            pltpu.VMEM((owners, 1, CAP), I32),
            pltpu.VMEM((parts, width, height), F32),
            pltpu.VMEM((6, parts, 8, width), F32),
            pltpu.VMEM((2, parts, 8, height), F32),
            pltpu.VMEM((2 * width + 8, height), BF16),
            pltpu.VMEM((2 * width + 8, height), BF16),
            pltpu.VMEM((2 * width + 8, LANES), F32),
            pltpu.VMEM((2 * width + 8, LANES), F32),
            dma, dma, dma, dma((groups,)), dma((groups,)), dma((8,)), dma((8,)),
        ],
        compiler_params=pltpu.CompilerParams(collective_id=0, has_side_effects=True),
        name="rebin",
    )(particles, dest_key.reshape(1, -1), cell_a.reshape(1, -1), cell_b.reshape(1, -1), velocity)
    return binned, binned_cell.reshape(-1)


def solution(mesh):
    sizes = tuple(mesh.shape[a] for a in AXES)
    in_specs = (P(None, AXES), P(AXES), P(AXES), P(AXES), P(None, "gx", ("gy", "gz")))
    out_specs = (P(None, AXES), P(AXES))
    return jax.shard_map(
        functools.partial(shards, sizes), mesh=mesh, in_specs=in_specs, out_specs=out_specs, check_vma=False
    )
```

```python
import functools

import jax
import jax.numpy as jnp
from jax import lax
from jax.experimental import pallas as pl
from jax.experimental.pallas import tpu as pltpu
from jax.sharding import PartitionSpec as P

AXES = ("gx", "gy", "gz")
MESH = pl.DeviceIdType.MESH
F32, BF16, I32 = jnp.float32, jnp.bfloat16, jnp.int32
CAP = 256
CHUNK = 1024
LANES = 128
step_length = 0.5


def quad_weights(frac):
    return (0.5 * frac * (frac - 1.0), 1.0 - frac * frac, 0.5 * frac * (frac + 1.0))


def two_parts(x):
    high = x.astype(BF16)
    return high, (x - high.astype(F32)).astype(BF16)


def sort_phase(
    part_ref, key_ref, a_ref, b_ref,
    pos_ref, acc_ref, sorted_ref, sorted_cell_ref, table_ref, table_smem, sem, owners, between,
):
    count = part_ref.shape[1]
    chunks = count // CHUNK

    owner_ids = lax.broadcasted_iota(I32, (owners, CHUNK), 0)

    def count_chunk(i, total):
        keys = key_ref[:, pl.ds(pl.multiple_of(i * CHUNK, CHUNK), CHUNK)]
        hot = (owner_ids == keys).astype(F32)
        for j in range(CHUNK // LANES):
            total = total + hot[:, j * LANES : (j + 1) * LANES]
        return total

    spread = lax.fori_loop(0, chunks, count_chunk, jnp.zeros((owners, LANES), F32))
    hist = jnp.broadcast_to(jnp.sum(spread, axis=1, keepdims=True), (owners, owners))
    row = lax.broadcasted_iota(I32, (owners, owners), 0)
    col = lax.broadcasted_iota(I32, (owners, owners), 1)
    below = (col < row).astype(F32).astype(BF16)
    starts = jnp.dot(below, hist.astype(BF16), preferred_element_type=F32)
    table_ref[0:8, :] = starts.T[0:8, :].astype(I32)
    table_ref[8:16, :] = hist.T[0:8, :].astype(I32)
    copy = pltpu.make_async_copy(table_ref, table_smem, sem)
    copy.start()

    upper = (
        lax.broadcasted_iota(I32, (CAP, CAP), 0) <= lax.broadcasted_iota(I32, (CAP, CAP), 1)
    ).astype(F32).astype(BF16)
    block_ids = lax.broadcasted_iota(I32, (owners, CAP), 0)

    def rank_chunk(i, base):
        for j in range(CHUNK // CAP):
            at = pl.ds(pl.multiple_of(i * CHUNK + j * CAP, CAP), CAP)
            hot = (block_ids == key_ref[:, at]).astype(F32)
            upto = jnp.dot(hot.astype(BF16), upper, preferred_element_type=F32)
            places = jnp.sum(hot * (upto + base), axis=0, keepdims=True) - 1.0
            pos_ref[:, at] = places.astype(I32)
            base = base + upto[:, CAP - 1 : CAP]
        return base

    lax.fori_loop(0, chunks, rank_chunk, starts[:, 0:1])
    between()

    acc_ref[...] = jnp.zeros_like(acc_ref)
    lane_ids = lax.broadcasted_iota(I32, (CAP, CHUNK), 0)
    page_ids = lax.broadcasted_iota(I32, (32, CHUNK), 0)

    def place_chunk(i, carry):
        at = pl.ds(pl.multiple_of(i * CHUNK, CHUNK), CHUNK)
        pos = pos_ref[:, at]
        page = pos >> 8
        lane_hot = (lane_ids == (pos & 255)).astype(F32).astype(BF16)
        values = jnp.concatenate(two_parts(part_ref[:, at]), axis=0)
        page16 = jnp.broadcast_to(page, (16, CHUNK)).astype(F32).astype(BF16)
        zero = jnp.zeros((16, CHUNK), BF16)
        rows = [jnp.where(page16 == BF16(h), values, zero) for h in range(32)]
        page_hot = (page_ids == page)
        rows.append(jnp.where(page_hot, a_ref[:, at].astype(F32), 0.0).astype(BF16))
        rows.append(jnp.where(page_hot, b_ref[:, at].astype(F32), 0.0).astype(BF16))
        acc_ref[...] += lax.dot_general(
            jnp.concatenate(rows, axis=0), lane_hot, (((1,), (1,)), ((), ())),
            preferred_element_type=F32,
        )
        return carry

    lax.fori_loop(0, chunks, place_chunk, 0)

    cells = (acc_ref[512:544, :] * 128.0 + acc_ref[544:576, :]).astype(I32)
    for h in range(32):
        both = acc_ref[16 * h : 16 * h + 8, :] + acc_ref[16 * h + 8 : 16 * h + 16, :]
        for j in range(2):
            sorted_ref[2 * h + j] = both[:, j * LANES : (j + 1) * LANES]
            sorted_cell_ref[2 * h + j] = cells[h : h + 1, j * LANES : (j + 1) * LANES]
    for j in range(64, 67):
        sorted_ref[j] = jnp.zeros((8, LANES), F32)
        sorted_cell_ref[j] = jnp.zeros((1, LANES), I32)
    copy.wait()


def expand(d, sorted_ref, sorted_cell_ref, table_smem, send_ref, send_cell_ref):
    lanes8 = lax.broadcasted_iota(I32, (8, LANES), 1)
    lanes1 = lax.broadcasted_iota(I32, (1, LANES), 1)
    start = jnp.clip(table_smem[0, d], 0, LANES * (sorted_ref.shape[0] - 3))
    live = table_smem[8, d]
    page = start >> 7
    shift = start & 127
    turn = (LANES - shift) & 127
    head8, head1 = lanes8 < LANES - shift, lanes1 < LANES - shift
    rolled = [pltpu.roll(sorted_ref[page + j], turn, 1) for j in range(3)]
    cell_rolled = [pltpu.roll(sorted_cell_ref[page + j], turn, 1) for j in range(3)]
    for j in range(2):
        here = slice(j * LANES, (j + 1) * LANES)
        value = jnp.where(head8, rolled[j], rolled[j + 1])
        send_ref[d, :, here] = jnp.where(lanes8 < live - j * LANES, value, 0.0)
        cell = jnp.where(head1, cell_rolled[j], cell_rolled[j + 1])
        send_cell_ref[d, :, here] = jnp.where(lanes1 < live - j * LANES, cell, -1)


def prepare_field(sizes, turned_ref, rows_ref, cols_ref, field_ref):
    nx, ny, nz = sizes
    width, height = turned_ref.shape[1], turned_ref.shape[2]
    x = lax.axis_index("gx")
    tile = lax.axis_index("gy") * nz + lax.axis_index("gz")
    has_left, has_right = tile > 0, tile < ny * nz - 1
    left = [jnp.where(has_left, cols_ref[0, c, 7:8, :], 0.0) for c in range(2)]
    right = [jnp.where(has_right, cols_ref[1, c, 0:1, :], 0.0) for c in range(2)]
    zeros = jnp.zeros((4, height), F32)
    sides = jnp.concatenate([left[0], right[0], left[1], right[1], zeros], axis=0)
    for c, at in ((0, 0), (1, width), (None, 2 * width)):
        block = sides if c is None else turned_ref[c]
        high, low = two_parts(block)
        here = slice(at, at + block.shape[0])
        field_ref[here, 0:height] = high
        field_ref[here, height : 2 * height] = high
        field_ref[here, 2 * height : 3 * height] = low
    lane = lax.broadcasted_iota(I32, (1, LANES), 1)
    pieces = [[], [], []]
    for first, row, there in ((0, 7, x > 0), (3, 0, x < nx - 1)):
        for c in range(2):
            tile8 = jnp.where(there, rows_ref[first + 1, c], 0.0)
            pieces[c].append(jnp.broadcast_to(tile8.T[:, row : row + 1], (width, LANES)))
        corner = []
        for c in range(2):
            from_left = rows_ref[first, c][row : row + 1, width - 1 : width]
            from_right = rows_ref[first + 2, c][row : row + 1, 0:1]
            corner.append(jnp.where(there & has_left, from_left, 0.0))
            corner.append(jnp.where(there & has_right, from_right, 0.0))
        corner = jnp.concatenate(corner + [jnp.zeros((4, 1), F32)], axis=0)
        pieces[2].append(jnp.broadcast_to(corner, (8, LANES)))
    for c in range(3):
        rows = pieces[c][0].shape[0]
        here = slice(c * width, c * width + rows)
        (up_high, up_low), (down_high, down_low) = (two_parts(v) for v in pieces[c])
        up_high, up_low, down_high, down_low = (v.astype(F32) for v in (up_high, up_low, down_high, down_low))
        up = jnp.where(lane == 47, up_low, jnp.where((lane == 15) | (lane == 31), up_high, 0.0))
        down = jnp.where(lane == 32, down_low, jnp.where((lane == 0) | (lane == 16), down_high, 0.0))
        field_ref[here, 3 * height : 3 * height + LANES] = (up + down).astype(BF16)


GROUP = 8
STEP = 4
SIDE = 4


def weight_rows(data, cell, sub16, height):
    node_a = jnp.where(cell >= 0, cell >> 7, 2 * height)
    below, same, above = quad_weights(data)
    parts = [two_parts(w[0:1, :]) for w in (below, same, above)]

    def wide(v):
        return jnp.broadcast_to(v, (16, CAP))

    def wide16(v):
        return wide(v.astype(F32).astype(BF16))

    a_in, a_page = node_a & 15, node_a >> 4
    a_next = jnp.where(a_in == 15, a_page + 1, jnp.where(a_in == 0, a_page - 1, -9))
    in16, page16, next16 = wide16(a_in), wide16(a_page), wide16(a_next)
    is_below, is_same, is_above = sub16 == in16 - BF16(1), sub16 == in16, sub16 == in16 + BF16(1)
    wrap_up, wrap_down = sub16 == in16 - BF16(15), sub16 == in16 + BF16(15)
    none = jnp.zeros((16, CAP), BF16)
    near, far = [], []
    for h in range(2):
        low, mid, high = (wide(p[h]) for p in parts)
        near.append(jnp.where(is_below, low, jnp.where(is_same, mid, jnp.where(is_above, high, none))))
        far.append(jnp.where(wrap_up, high, jnp.where(wrap_down, low, none)))
    return near, far, page16, next16, none


def build_weights(data, cell, weight_ref, lanes, height):
    sub16 = lax.broadcasted_iota(I32, (16, CAP), 0).astype(F32).astype(BF16)
    near, far, page16, next16, none = weight_rows(data, cell, sub16, height)
    for c in range(height // 16):
        here_c, next_c = page16 == BF16(c), next16 == BF16(c)
        for h in range(2):
            rows = jnp.where(here_c, near[h], jnp.where(next_c, far[h], none))
            at = h * height + 16 * c
            weight_ref[at : at + 16, lanes] = rows
    out_c = (next16 == BF16(-1)) | (next16 == BF16(height // 16))
    for k, h in enumerate((0, 1, 0)):
        at = 2 * height + 16 * k
        weight_ref[at : at + 16, lanes] = jnp.where(out_c, far[h], none)


def mix(field_ref, weight_ref, height):
    weights = weight_ref[...]
    stacked = jnp.concatenate([weights[0 : 2 * height], weights[0:height], weights[2 * height :]], axis=0)
    return jnp.dot(field_ref[:, 0 : 3 * height + 48], stacked, preferred_element_type=F32)


def pick_columns(data, cell, mixed_ref, lanes, width):
    sub8 = lax.broadcasted_iota(I32, (8, CAP), 0)
    node_b = cell & 127
    trio = quad_weights(data)

    def wide(v):
        return jnp.broadcast_to(v, (8, CAP))

    low, mid, high = (wide(w[1:2, :]) for w in trio)
    b_in, b_page = wide(node_b & 7), wide(node_b >> 3)
    b_next = jnp.where(b_in == 7, b_page + 1, jnp.where(b_in == 0, b_page - 1, -9))
    near = jnp.where(sub8 == b_in - 1, low, jnp.where(sub8 == b_in, mid, jnp.where(sub8 == b_in + 1, high, 0.0)))
    far = jnp.where(sub8 == b_in - 7, high, jnp.where(sub8 == b_in + 7, low, 0.0))
    picked = [[jnp.zeros((8, CAP), F32)] * 2 for _ in range(2)]
    for c in range(width // 8):
        here_c, next_c = b_page == c, b_next == c
        for k in range(2):
            at = k * width + 8 * c
            block = mixed_ref[at : at + 8, lanes]
            picked[k][0] = jnp.where(here_c, block, picked[k][0])
            picked[k][1] = jnp.where(next_c, block, picked[k][1])
    speed = []
    for k in range(2):
        side = 2 * width + 2 * k
        other = jnp.where(b_next == -1, wide(mixed_ref[side : side + 1, lanes]), picked[k][1])
        other = jnp.where(b_next == width // 8, wide(mixed_ref[side + 1 : side + 2, lanes]), other)
        speed.append(jnp.sum(picked[k][0] * near + other * far, axis=0, keepdims=True))
    shift = jnp.where(sub8 == 2, speed[0], jnp.where(sub8 == 3, speed[1], 0.0))
    return data + step_length * shift


def build_step(base, arrived_ref, cell_ref, weight_ref, height):
    for i in range(STEP):
        s = base + i
        here = pl.ds(pl.multiple_of(s * CAP, CAP), CAP)
        lanes = slice(i * CAP, (i + 1) * CAP)
        build_weights(arrived_ref[:, here], cell_ref[s], weight_ref, lanes, height)


def pick_step(base, arrived_ref, cell_ref, out_ref, mixed_ref, width):
    for i in range(STEP):
        s = base + i
        here = pl.ds(pl.multiple_of(s * CAP, CAP), CAP)
        lanes = slice(i * CAP, (i + 1) * CAP)
        out_ref[:, here] = pick_columns(arrived_ref[:, here], cell_ref[s], mixed_ref, lanes, width)


def wrapped(at, step, length):
    to = at + step
    return jnp.where(to >= length, to - length, to)


def rebin_kernel(
    sizes, part_ref, key_ref, a_ref, b_ref, vel_ref, out_ref, cell_ref,
    pos_ref, acc_ref, sorted_ref, sorted_cell_ref, table_ref, table_smem,
    send_ref, send_cell_ref, turned_ref, rows_ref, cols_ref, field_ref, arrived_ref,
    weight0_ref, weight1_ref, mixed0_ref, mixed1_ref,
    table_sem, send_sem, send_cell_sem, recv_sem, recv_cell_sem, halo_send, halo_recv,
):
    nx, ny, nz = sizes
    total = nx * ny * nz
    x, y, z = (lax.axis_index(a) for a in AXES)
    me = (x * ny + y) * nz + z
    tiles = ny * nz
    tile = y * nz + z
    height, width = vel_ref.shape[1], vel_ref.shape[2]
    outer, inner = y // SIDE, y % SIDE
    steps = [(a, b) for a in (2, 3, 0, 1) for b in (2, 3, 0, 1)]
    ahead_x = [wrapped(x, d, nx) for d in range(nx)]
    ahead_y = [wrapped(outer, d, ny // SIDE) for d in range(ny // SIDE)]
    ahead_i = [wrapped(inner, d, SIDE) for d in range(SIDE)]
    ahead_z = [z, 1 - z]

    barrier = pltpu.get_barrier_semaphore()
    for a, b in steps:
        for i in range(SIDE):
            for c in range(nz):
                if (a, b, i, c) != (0, 0, 0, 0):
                    device = (ahead_x[a], ahead_y[b] * SIDE + ahead_i[i], ahead_z[c])
                    pl.semaphore_signal(barrier, inc=1, device_id=device, device_id_type=MESH)
    turned_ref[0] = vel_ref[0].T
    turned_ref[1] = vel_ref[1].T

    halos = []
    for i, dx in enumerate((1, nx - 1)):
        edge = vel_ref.at[:, pl.ds(height - 8 if dx == 1 else 0, 8), :]
        for j, dt in enumerate((1, 0, tiles - 1)):
            halos.append((edge, rows_ref.at[3 * i + j], ahead_x[dx], wrapped(tile, dt, tiles)))
    for i, dt in enumerate((1, tiles - 1)):
        edge = turned_ref.at[:, pl.ds(width - 8 if dt == 1 else 0, 8), :]
        halos.append((edge, cols_ref.at[i], x, wrapped(tile, dt, tiles)))
    halo_copies = [
        pltpu.make_async_remote_copy(
            src_ref=src, dst_ref=dst, send_sem=halo_send.at[k], recv_sem=halo_recv.at[k],
            device_id=(to_x, to_t // nz, to_t % nz), device_id_type=MESH,
        )
        for k, (src, dst, to_x, to_t) in enumerate(halos)
    ]

    def between():
        pl.semaphore_wait(barrier, total - 1)
        for c in halo_copies:
            c.start()

    sort_phase(
        part_ref, key_ref, a_ref, b_ref, pos_ref, acc_ref, sorted_ref, sorted_cell_ref,
        table_ref, table_smem, table_sem, total, between,
    )

    mine = pl.ds(pl.multiple_of(me * CAP, CAP), CAP)

    def first_of(a, b):
        return (ahead_x[a] * (ny // SIDE) + ahead_y[b]) * GROUP

    def send_group(g):
        a, b = steps[g]
        for i in range(SIDE):
            for c in range(nz):
                there = first_of(a, b) + ahead_i[i] * nz + ahead_z[c]
                if (a, b, i, c) == (0, 0, 0, 0):
                    pltpu.make_async_copy(send_ref.at[there], arrived_ref.at[:, mine], recv_sem.at[g]).start()
                    pltpu.make_async_copy(send_cell_ref.at[there], cell_ref.at[me], recv_cell_sem.at[g]).start()
                    continue
                device = (ahead_x[a], ahead_y[b] * SIDE + ahead_i[i], ahead_z[c])
                pltpu.make_async_remote_copy(
                    src_ref=send_ref.at[there], dst_ref=arrived_ref.at[:, mine], send_sem=send_sem,
                    recv_sem=recv_sem.at[g], device_id=device, device_id_type=MESH,
                ).start()
                pltpu.make_async_remote_copy(
                    src_ref=send_cell_ref.at[there], dst_ref=cell_ref.at[me], send_sem=send_cell_sem,
                    recv_sem=recv_cell_sem.at[g], device_id=device, device_id_type=MESH,
                ).start()

    for g, (a, b) in enumerate(steps):
        base = first_of(a, b)

        def expand_one(i, carry, base=base):
            expand(base + i, sorted_ref, sorted_cell_ref, table_smem, send_ref, send_cell_ref)
            return carry

        lax.fori_loop(0, GROUP, expand_one, 0, unroll=True)
        if g > 0:
            send_group(g - 1)
    groups = len(steps)
    send_group(groups - 1)

    for c in halo_copies:
        c.wait()
    prepare_field(sizes, turned_ref, rows_ref, cols_ref, field_ref)

    def source_base(g):
        back_x = (x + 2 * nx - 2 - g // 4) % nx
        back_y = (outer + 2 * (ny // SIDE) - 2 - g % 4) % (ny // SIDE)
        return (back_x * (ny // SIDE) + back_y) * GROUP

    def arrive(g):
        blocks = arrived_ref.at[:, pl.ds(0, GROUP * CAP)]
        pltpu.make_async_copy(blocks, blocks, recv_sem.at[g]).wait()
        few = cell_ref.at[pl.ds(0, GROUP)]
        pltpu.make_async_copy(few, few, recv_cell_sem.at[g]).wait()

    build = lambda base, ref: build_step(base, arrived_ref, cell_ref, ref, height)
    pick = lambda base, ref: pick_step(base, arrived_ref, cell_ref, out_ref, ref, width)
    arrive(0)
    start = source_base(0)
    build(start, weight0_ref)
    mixed0_ref[...] = mix(field_ref, weight0_ref, height)
    build(start + STEP, weight1_ref)

    def one_group(g, before):
        arrive(g)
        base = source_base(g)
        mixed1_ref[...] = mix(field_ref, weight1_ref, height)
        pick(before, mixed0_ref)
        build(base, weight0_ref)
        mixed0_ref[...] = mix(field_ref, weight0_ref, height)
        pick(before + STEP, mixed1_ref)
        build(base + STEP, weight1_ref)
        return base

    last = lax.fori_loop(1, groups, one_group, start)
    mixed1_ref[...] = mix(field_ref, weight1_ref, height)
    pick(last, mixed0_ref)
    pick(last + STEP, mixed1_ref)
    some = send_ref.at[pl.ds(0, total - 1)]
    some_cell = send_cell_ref.at[pl.ds(0, total - 1)]
    pltpu.make_async_copy(some, some, send_sem).wait()
    pltpu.make_async_copy(some_cell, some_cell, send_cell_sem).wait()


def shards(sizes, particles, dest_key, cell_a, cell_b, velocity):
    owners = sizes[0] * sizes[1] * sizes[2]
    count = particles.shape[1]
    parts, height, width = velocity.shape
    vmem = pl.BlockSpec(memory_space=pltpu.VMEM)
    dma = pltpu.SemaphoreType.DMA
    groups = owners // GROUP
    binned, binned_cell = pl.pallas_call(
        functools.partial(rebin_kernel, sizes),
        out_shape=(
            jax.ShapeDtypeStruct((8, owners * CAP), F32),
            jax.ShapeDtypeStruct((owners, 1, CAP), I32),
        ),
        in_specs=[vmem] * 5,
        out_specs=(vmem,) * 2,
        scratch_shapes=[
            pltpu.VMEM((1, count), I32),
            pltpu.VMEM((576, CAP), F32),
            pltpu.VMEM((67, 8, LANES), F32),
            pltpu.VMEM((67, 1, LANES), I32),
            pltpu.VMEM((16, LANES), I32),
            pltpu.SMEM((16, LANES), I32),
            pltpu.VMEM((owners, 8, CAP), F32),
            pltpu.VMEM((owners, 1, CAP), I32),
            pltpu.VMEM((parts, width, height), F32),
            pltpu.VMEM((6, parts, 8, width), F32),
            pltpu.VMEM((2, parts, 8, height), F32),
            pltpu.VMEM((2 * width + 8, 3 * height + LANES), BF16),
            pltpu.VMEM((8, owners * CAP), F32),
            pltpu.VMEM((2 * height + 48, STEP * CAP), BF16),
            pltpu.VMEM((2 * height + 48, STEP * CAP), BF16),
            pltpu.VMEM((2 * width + 8, STEP * CAP), F32),
            pltpu.VMEM((2 * width + 8, STEP * CAP), F32),
            dma, dma, dma, dma((groups,)), dma((groups,)), dma((8,)), dma((8,)),
        ],
        compiler_params=pltpu.CompilerParams(collective_id=0, has_side_effects=True),
        name="rebin",
    )(particles, dest_key.reshape(1, -1), cell_a.reshape(1, -1), cell_b.reshape(1, -1), velocity)
    return binned, binned_cell.reshape(-1)


def solution(mesh):
    sizes = tuple(mesh.shape[a] for a in AXES)
    in_specs = (P(None, AXES), P(AXES), P(AXES), P(AXES), P(None, "gx", ("gy", "gz")))
    out_specs = (P(None, AXES), P(AXES))
    return jax.shard_map(
        functools.partial(shards, sizes), mesh=mesh, in_specs=in_specs, out_specs=out_specs, check_vma=False
    )
```

```python
import functools

import jax
import jax.numpy as jnp
from jax import lax
from jax.experimental import pallas as pl
from jax.experimental.pallas import tpu as pltpu
from jax.sharding import PartitionSpec as P

AXES = ("gx", "gy", "gz")
MESH = pl.DeviceIdType.MESH
F32, BF16, I32 = jnp.float32, jnp.bfloat16, jnp.int32
CAP = 256
CHUNK = 2048
LANES = 128
step_length = 0.5


def quad_weights(frac):
    return (0.5 * frac * (frac - 1.0), 1.0 - frac * frac, 0.5 * frac * (frac + 1.0))


def two_parts(x):
    high = x.astype(BF16)
    return high, (x - high.astype(F32)).astype(BF16)


def sort_phase(
    part_ref, key_ref, a_ref, b_ref,
    pos_ref, acc_ref, sorted_ref, sorted_cell_ref, table_ref, table_smem, sem, owners, between,
):
    count = part_ref.shape[1]
    chunks = count // CHUNK

    owner_ids = lax.broadcasted_iota(I32, (owners, CHUNK), 0)

    def count_chunk(i, total):
        keys = key_ref[:, pl.ds(pl.multiple_of(i * CHUNK, CHUNK), CHUNK)]
        hot = (owner_ids == keys).astype(F32)
        for j in range(CHUNK // LANES):
            total = total + hot[:, j * LANES : (j + 1) * LANES]
        return total

    spread = lax.fori_loop(0, chunks, count_chunk, jnp.zeros((owners, LANES), F32), unroll=True)
    hist = jnp.broadcast_to(jnp.sum(spread, axis=1, keepdims=True), (owners, owners))
    row = lax.broadcasted_iota(I32, (owners, owners), 0)
    col = lax.broadcasted_iota(I32, (owners, owners), 1)
    below = (col < row).astype(F32).astype(BF16)
    starts = jnp.dot(below, hist.astype(BF16), preferred_element_type=F32)
    table_ref[0:8, :] = starts.T[0:8, :].astype(I32)
    table_ref[8:16, :] = hist.T[0:8, :].astype(I32)
    copy = pltpu.make_async_copy(table_ref, table_smem, sem)
    copy.start()

    upper = (
        lax.broadcasted_iota(I32, (CAP, CAP), 0) <= lax.broadcasted_iota(I32, (CAP, CAP), 1)
    ).astype(F32).astype(BF16)
    block_ids = lax.broadcasted_iota(I32, (owners, CAP), 0)

    def rank_chunk(i, base):
        for j in range(CHUNK // CAP):
            at = pl.ds(pl.multiple_of(i * CHUNK + j * CAP, CAP), CAP)
            hot = (block_ids == key_ref[:, at]).astype(F32)
            upto = jnp.dot(hot.astype(BF16), upper, preferred_element_type=F32)
            places = jnp.sum(hot * (upto + base), axis=0, keepdims=True) - 1.0
            pos_ref[:, at] = places.astype(I32)
            base = base + upto[:, CAP - 1 : CAP]
        return base

    lax.fori_loop(0, chunks, rank_chunk, starts[:, 0:1], unroll=True)
    between()

    acc_ref[...] = jnp.zeros_like(acc_ref)
    lane_ids = lax.broadcasted_iota(I32, (CAP, CHUNK), 0)
    page_ids = lax.broadcasted_iota(I32, (32, CHUNK), 0)

    def place_chunk(i, carry):
        at = pl.ds(pl.multiple_of(i * CHUNK, CHUNK), CHUNK)
        pos = pos_ref[:, at]
        page = pos >> 8
        lane_hot = (lane_ids == (pos & 255)).astype(F32).astype(BF16)
        values = jnp.concatenate(two_parts(part_ref[:, at]), axis=0)
        page16 = jnp.broadcast_to(page, (16, CHUNK)).astype(F32).astype(BF16)
        zero = jnp.zeros((16, CHUNK), BF16)
        rows = [jnp.where(page16 == BF16(h), values, zero) for h in range(32)]
        page_hot = (page_ids == page)
        rows.append(jnp.where(page_hot, a_ref[:, at].astype(F32), 0.0).astype(BF16))
        rows.append(jnp.where(page_hot, b_ref[:, at].astype(F32), 0.0).astype(BF16))
        acc_ref[...] += lax.dot_general(
            jnp.concatenate(rows, axis=0), lane_hot, (((1,), (1,)), ((), ())),
            preferred_element_type=F32,
        )
        return carry

    lax.fori_loop(0, chunks, place_chunk, 0, unroll=True)

    cells = (acc_ref[512:544, :] * 128.0 + acc_ref[544:576, :]).astype(I32)
    for h in range(32):
        both = acc_ref[16 * h : 16 * h + 8, :] + acc_ref[16 * h + 8 : 16 * h + 16, :]
        for j in range(2):
            sorted_ref[2 * h + j] = both[:, j * LANES : (j + 1) * LANES]
            sorted_cell_ref[2 * h + j] = cells[h : h + 1, j * LANES : (j + 1) * LANES]
    for j in range(64, 67):
        sorted_ref[j] = jnp.zeros((8, LANES), F32)
        sorted_cell_ref[j] = jnp.zeros((1, LANES), I32)
    copy.wait()


def expand(d, sorted_ref, sorted_cell_ref, table_smem, send_ref, send_cell_ref):
    lanes8 = lax.broadcasted_iota(I32, (8, LANES), 1)
    lanes1 = lax.broadcasted_iota(I32, (1, LANES), 1)
    start = jnp.clip(table_smem[0, d], 0, LANES * (sorted_ref.shape[0] - 3))
    live = table_smem[8, d]
    page = start >> 7
    shift = start & 127
    turn = (LANES - shift) & 127
    head8, head1 = lanes8 < LANES - shift, lanes1 < LANES - shift
    rolled = [pltpu.roll(sorted_ref[page + j], turn, 1) for j in range(3)]
    cell_rolled = [pltpu.roll(sorted_cell_ref[page + j], turn, 1) for j in range(3)]
    for j in range(2):
        here = slice(j * LANES, (j + 1) * LANES)
        value = jnp.where(head8, rolled[j], rolled[j + 1])
        send_ref[d, :, here] = jnp.where(lanes8 < live - j * LANES, value, 0.0)
        cell = jnp.where(head1, cell_rolled[j], cell_rolled[j + 1])
        send_cell_ref[d, :, here] = jnp.where(lanes1 < live - j * LANES, cell, -1)


def prepare_field(sizes, turned_ref, rows_ref, cols_ref, field_ref, up_ref, down_ref):
    nx, ny, nz = sizes
    width, height = turned_ref.shape[1], turned_ref.shape[2]
    x = lax.axis_index("gx")
    tile = lax.axis_index("gy") * nz + lax.axis_index("gz")
    has_left, has_right = tile > 0, tile < ny * nz - 1
    left = [jnp.where(has_left, cols_ref[0, c, 7:8, :], 0.0) for c in range(2)]
    right = [jnp.where(has_right, cols_ref[1, c, 0:1, :], 0.0) for c in range(2)]
    zeros = jnp.zeros((4, height), F32)
    sides = jnp.concatenate([left[0], right[0], left[1], right[1], zeros], axis=0)
    for c, at in ((0, 0), (1, width), (None, 2 * width)):
        block = sides if c is None else turned_ref[c]
        high, low = two_parts(block)
        here = slice(at, at + block.shape[0])
        field_ref[here, 0:height] = high
        field_ref[here, height : 2 * height] = high
        field_ref[here, 2 * height : 3 * height] = low
    for ref, first, row, there in ((up_ref, 0, 7, x > 0), (down_ref, 3, 0, x < nx - 1)):
        corner = []
        for c in range(2):
            tile8 = jnp.where(there, rows_ref[first + 1, c], 0.0)
            line = tile8.T[:, row : row + 1]
            ref[c * width : (c + 1) * width, :] = jnp.broadcast_to(line, (width, LANES))
            from_left = rows_ref[first, c][row : row + 1, width - 1 : width]
            from_right = rows_ref[first + 2, c][row : row + 1, 0:1]
            corner.append(jnp.where(there & has_left, from_left, 0.0))
            corner.append(jnp.where(there & has_right, from_right, 0.0))
        corner = jnp.concatenate(corner + [jnp.zeros((4, 1), F32)], axis=0)
        ref[2 * width :, :] = jnp.broadcast_to(corner, (8, LANES))


GROUP = 8
STEP = 4
SIDE = 4


def weight_rows(data, cell, sub16, height):
    node_a = jnp.where(cell >= 0, cell >> 7, 2 * height)
    below, same, above = quad_weights(data)
    parts = [two_parts(w[0:1, :]) for w in (below, same, above)]

    def wide(v):
        return jnp.broadcast_to(v, (16, CAP))

    def wide16(v):
        return wide(v.astype(F32).astype(BF16))

    a_in, a_page = node_a & 15, node_a >> 4
    a_next = jnp.where(a_in == 15, a_page + 1, jnp.where(a_in == 0, a_page - 1, -9))
    in16, page16, next16 = wide16(a_in), wide16(a_page), wide16(a_next)
    is_below, is_same, is_above = sub16 == in16 - BF16(1), sub16 == in16, sub16 == in16 + BF16(1)
    wrap_up, wrap_down = sub16 == in16 - BF16(15), sub16 == in16 + BF16(15)
    none = jnp.zeros((16, CAP), BF16)
    near, far = [], []
    for h in range(2):
        low, mid, high = (wide(p[h]) for p in parts)
        near.append(jnp.where(is_below, low, jnp.where(is_same, mid, jnp.where(is_above, high, none))))
        far.append(jnp.where(wrap_up, high, jnp.where(wrap_down, low, none)))
    return near, far, page16, next16, none


def build_weights(data, cell, weight_ref, lanes, height):
    sub16 = lax.broadcasted_iota(I32, (16, CAP), 0).astype(F32).astype(BF16)
    near, far, page16, next16, none = weight_rows(data, cell, sub16, height)
    for c in range(height // 16):
        here_c, next_c = page16 == BF16(c), next16 == BF16(c)
        for h in range(2):
            rows = jnp.where(here_c, near[h], jnp.where(next_c, far[h], none))
            at = h * height + 16 * c
            weight_ref[at : at + 16, lanes] = rows


def mix(field_ref, weight_ref, height):
    weights = weight_ref[...]
    stacked = jnp.concatenate([weights, weights[0:height]], axis=0)
    return jnp.dot(field_ref[...], stacked, preferred_element_type=F32)


def pick_columns(data, cell, mixed_ref, up_ref, down_ref, lanes, height, width):
    sub8 = lax.broadcasted_iota(I32, (8, CAP), 0)
    node_b = cell & 127
    trio = quad_weights(data)

    def wide(v):
        return jnp.broadcast_to(v, (8, CAP))

    low, mid, high = (wide(w[1:2, :]) for w in trio)
    b_in, b_page = wide(node_b & 7), wide(node_b >> 3)
    b_next = jnp.where(b_in == 7, b_page + 1, jnp.where(b_in == 0, b_page - 1, -9))
    near = jnp.where(sub8 == b_in - 1, low, jnp.where(sub8 == b_in, mid, jnp.where(sub8 == b_in + 1, high, 0.0)))
    far = jnp.where(sub8 == b_in - 7, high, jnp.where(sub8 == b_in + 7, low, 0.0))
    first = cell < width
    edge = jnp.where(first, trio[0][0:1, :], jnp.where(cell >= (height - 1) * width, trio[2][0:1, :], 0.0))
    edge, first = wide(jnp.where(cell >= 0, edge, 0.0)), wide(cell) < width

    def rows_at(at):
        up = jnp.concatenate([up_ref[at : at + 8, :]] * 2, axis=1)
        down = jnp.concatenate([down_ref[at : at + 8, :]] * 2, axis=1)
        return mixed_ref[at : at + 8, lanes] + jnp.where(first, up, down) * edge

    picked = [[jnp.zeros((8, CAP), F32)] * 2 for _ in range(2)]
    for c in range(width // 8):
        here_c, next_c = b_page == c, b_next == c
        for k in range(2):
            block = rows_at(k * width + 8 * c)
            picked[k][0] = jnp.where(here_c, block, picked[k][0])
            picked[k][1] = jnp.where(next_c, block, picked[k][1])
    speed = []
    sides = rows_at(2 * width)
    for k in range(2):
        other = jnp.where(b_next == -1, wide(sides[2 * k : 2 * k + 1, :]), picked[k][1])
        other = jnp.where(b_next == width // 8, wide(sides[2 * k + 1 : 2 * k + 2, :]), other)
        speed.append(jnp.sum(picked[k][0] * near + other * far, axis=0, keepdims=True))
    shift = jnp.where(sub8 == 2, speed[0], jnp.where(sub8 == 3, speed[1], 0.0))
    return data + step_length * shift


def build_step(base, arrived_ref, cell_ref, weight_ref, height):
    for i in range(STEP):
        s = base + i
        here = pl.ds(pl.multiple_of(s * CAP, CAP), CAP)
        lanes = slice(i * CAP, (i + 1) * CAP)
        build_weights(arrived_ref[:, here], cell_ref[s], weight_ref, lanes, height)


def pick_step(base, arrived_ref, cell_ref, out_ref, mixed_ref, up_ref, down_ref, height, width):
    for i in range(STEP):
        s = base + i
        here = pl.ds(pl.multiple_of(s * CAP, CAP), CAP)
        lanes = slice(i * CAP, (i + 1) * CAP)
        out_ref[:, here] = pick_columns(
            arrived_ref[:, here], cell_ref[s], mixed_ref, up_ref, down_ref, lanes, height, width
        )


def wrapped(at, step, length):
    to = at + step
    return jnp.where(to >= length, to - length, to)


def rebin_kernel(
    sizes, part_in, key_in, a_in, b_in, vel_in, out_ref, cell_ref,
    part_ref, key_ref, a_ref, b_ref, vel_ref,
    pos_ref, acc_ref, sorted_ref, sorted_cell_ref, table_ref, table_smem,
    send_ref, send_cell_ref, turned_ref, rows_ref, cols_ref, field_ref, up_ref, down_ref, arrived_ref,
    weight0_ref, weight1_ref, mixed0_ref, mixed1_ref,
    load_sem, table_sem, send_sem, send_cell_sem, recv_sem, recv_cell_sem, halo_send, halo_recv,
):
    nx, ny, nz = sizes
    total = nx * ny * nz
    pairs = ((key_in, key_ref), (vel_in, vel_ref), (part_in, part_ref), (a_in, a_ref), (b_in, b_ref))
    loads = [pltpu.make_async_copy(src, dst, load_sem.at[k]) for k, (src, dst) in enumerate(pairs)]
    for load in loads:
        load.start()
    x, y, z = (lax.axis_index(a) for a in AXES)
    me = (x * ny + y) * nz + z
    tiles = ny * nz
    tile = y * nz + z
    height, width = vel_ref.shape[1], vel_ref.shape[2]
    outer, inner = y // SIDE, y % SIDE
    steps = [(0, 0), (0, 1), (1, 0), (0, 3), (3, 0), (1, 1), (3, 3), (1, 3), (3, 1), (0, 2), (2, 0), (1, 2), (2, 1), (3, 2), (2, 3), (2, 2)]
    ahead_x = [wrapped(x, d, nx) for d in range(nx)]
    ahead_y = [wrapped(outer, d, ny // SIDE) for d in range(ny // SIDE)]
    ahead_i = [wrapped(inner, d, SIDE) for d in range(SIDE)]
    ahead_z = [z, 1 - z]

    barrier = pltpu.get_barrier_semaphore()
    for a, b in steps:
        for i in range(SIDE):
            for c in range(nz):
                if (a, b, i, c) != (0, 0, 0, 0):
                    device = (ahead_x[a], ahead_y[b] * SIDE + ahead_i[i], ahead_z[c])
                    pl.semaphore_signal(barrier, inc=1, device_id=device, device_id_type=MESH)

    halos = []
    for i, dx in enumerate((1, nx - 1)):
        edge = vel_ref.at[:, pl.ds(height - 8 if dx == 1 else 0, 8), :]
        for j, dt in enumerate((1, 0, tiles - 1)):
            halos.append((edge, rows_ref.at[3 * i + j], ahead_x[dx], wrapped(tile, dt, tiles)))
    for i, dt in enumerate((1, tiles - 1)):
        edge = turned_ref.at[:, pl.ds(width - 8 if dt == 1 else 0, 8), :]
        halos.append((edge, cols_ref.at[i], x, wrapped(tile, dt, tiles)))
    halo_copies = [
        pltpu.make_async_remote_copy(
            src_ref=src, dst_ref=dst, send_sem=halo_send.at[k], recv_sem=halo_recv.at[k],
            device_id=(to_x, to_t // nz, to_t % nz), device_id_type=MESH,
        )
        for k, (src, dst, to_x, to_t) in enumerate(halos)
    ]

    def between():
        loads[1].wait()
        turned_ref[0] = vel_ref[0].T
        turned_ref[1] = vel_ref[1].T
        pl.semaphore_wait(barrier, total - 1)
        for c in halo_copies:
            c.start()
        for load in loads[2:]:
            load.wait()

    loads[0].wait()
    sort_phase(
        part_ref, key_ref, a_ref, b_ref, pos_ref, acc_ref, sorted_ref, sorted_cell_ref,
        table_ref, table_smem, table_sem, total, between,
    )

    mine = pl.ds(pl.multiple_of(me * CAP, CAP), CAP)

    def first_of(a, b):
        return (ahead_x[a] * (ny // SIDE) + ahead_y[b]) * GROUP

    def send_group(g):
        a, b = steps[g]
        for i in range(SIDE):
            for c in range(nz):
                there = first_of(a, b) + ahead_i[i] * nz + ahead_z[c]
                if (a, b, i, c) == (0, 0, 0, 0):
                    pltpu.make_async_copy(send_ref.at[there], arrived_ref.at[:, mine], recv_sem.at[g]).start()
                    pltpu.make_async_copy(send_cell_ref.at[there], cell_ref.at[me], recv_cell_sem.at[g]).start()
                    continue
                device = (ahead_x[a], ahead_y[b] * SIDE + ahead_i[i], ahead_z[c])
                pltpu.make_async_remote_copy(
                    src_ref=send_ref.at[there], dst_ref=arrived_ref.at[:, mine], send_sem=send_sem,
                    recv_sem=recv_sem.at[g], device_id=device, device_id_type=MESH,
                ).start()
                pltpu.make_async_remote_copy(
                    src_ref=send_cell_ref.at[there], dst_ref=cell_ref.at[me], send_sem=send_cell_sem,
                    recv_sem=recv_cell_sem.at[g], device_id=device, device_id_type=MESH,
                ).start()

    for g, (a, b) in enumerate(steps):
        base = first_of(a, b)

        def expand_one(i, carry, base=base):
            expand(base + i, sorted_ref, sorted_cell_ref, table_smem, send_ref, send_cell_ref)
            return carry

        lax.fori_loop(0, GROUP, expand_one, 0, unroll=True)
        if g > 0:
            send_group(g - 1)
    groups = len(steps)
    send_group(groups - 1)

    for c in halo_copies:
        c.wait()
    prepare_field(sizes, turned_ref, rows_ref, cols_ref, field_ref, up_ref, down_ref)

    def source_base(g):
        shift = jnp.int32(2) * g
        step_x = lax.shift_right_arithmetic(jnp.int32(-1369213168), shift) & 3
        step_y = lax.shift_right_arithmetic(jnp.int32(-1182141244), shift) & 3
        back_x = (x + nx - step_x) % nx
        back_y = (outer + ny // SIDE - step_y) % (ny // SIDE)
        return (back_x * (ny // SIDE) + back_y) * GROUP

    def arrive(g):
        blocks = arrived_ref.at[:, pl.ds(0, GROUP * CAP)]
        pltpu.make_async_copy(blocks, blocks, recv_sem.at[g]).wait()
        few = cell_ref.at[pl.ds(0, GROUP)]
        pltpu.make_async_copy(few, few, recv_cell_sem.at[g]).wait()

    build = lambda base, ref: build_step(base, arrived_ref, cell_ref, ref, height)
    pick = lambda base, ref: pick_step(
        base, arrived_ref, cell_ref, out_ref, ref, up_ref, down_ref, height, width
    )
    arrive(0)
    start = source_base(0)
    build(start, weight0_ref)
    mixed0_ref[...] = mix(field_ref, weight0_ref, height)
    build(start + STEP, weight1_ref)

    def one_group(g, before):
        arrive(g)
        base = source_base(g)
        mixed1_ref[...] = mix(field_ref, weight1_ref, height)
        pick(before, mixed0_ref)
        build(base, weight0_ref)
        mixed0_ref[...] = mix(field_ref, weight0_ref, height)
        pick(before + STEP, mixed1_ref)
        build(base + STEP, weight1_ref)
        return base

    last = lax.fori_loop(1, groups, one_group, start)
    mixed1_ref[...] = mix(field_ref, weight1_ref, height)
    pick(last, mixed0_ref)
    pick(last + STEP, mixed1_ref)
    some = send_ref.at[pl.ds(0, total - 1)]
    some_cell = send_cell_ref.at[pl.ds(0, total - 1)]
    pltpu.make_async_copy(some, some, send_sem).wait()
    pltpu.make_async_copy(some_cell, some_cell, send_cell_sem).wait()


def shards(sizes, particles, dest_key, cell_a, cell_b, velocity):
    owners = sizes[0] * sizes[1] * sizes[2]
    count = particles.shape[1]
    parts, height, width = velocity.shape
    vmem = pl.BlockSpec(memory_space=pltpu.VMEM)
    dma = pltpu.SemaphoreType.DMA
    groups = owners // GROUP
    binned, binned_cell = pl.pallas_call(
        functools.partial(rebin_kernel, sizes),
        out_shape=(
            jax.ShapeDtypeStruct((8, owners * CAP), F32),
            jax.ShapeDtypeStruct((owners, 1, CAP), I32),
        ),
        in_specs=[pl.BlockSpec(memory_space=pltpu.HBM)] * 5,
        out_specs=(vmem,) * 2,
        scratch_shapes=[
            pltpu.VMEM(particles.shape, F32),
            pltpu.VMEM((1, count), I32),
            pltpu.VMEM((1, count), I32),
            pltpu.VMEM((1, count), I32),
            pltpu.VMEM(velocity.shape, F32),
            pltpu.VMEM((1, count), I32),
            pltpu.VMEM((576, CAP), F32),
            pltpu.VMEM((67, 8, LANES), F32),
            pltpu.VMEM((67, 1, LANES), I32),
            pltpu.VMEM((16, LANES), I32),
            pltpu.SMEM((16, LANES), I32),
            pltpu.VMEM((owners, 8, CAP), F32),
            pltpu.VMEM((owners, 1, CAP), I32),
            pltpu.VMEM((parts, width, height), F32),
            pltpu.VMEM((6, parts, 8, width), F32),
            pltpu.VMEM((2, parts, 8, height), F32),
            pltpu.VMEM((2 * width + 8, 3 * height), BF16),
            pltpu.VMEM((2 * width + 8, LANES), F32),
            pltpu.VMEM((2 * width + 8, LANES), F32),
            pltpu.VMEM((8, owners * CAP), F32),
            pltpu.VMEM((2 * height, STEP * CAP), BF16),
            pltpu.VMEM((2 * height, STEP * CAP), BF16),
            pltpu.VMEM((2 * width + 8, STEP * CAP), F32),
            pltpu.VMEM((2 * width + 8, STEP * CAP), F32),
            dma((5,)), dma, dma, dma, dma((groups,)), dma((groups,)), dma((8,)), dma((8,)),
        ],
        compiler_params=pltpu.CompilerParams(collective_id=0, has_side_effects=True),
        name="rebin",
    )(particles, dest_key.reshape(1, -1), cell_a.reshape(1, -1), cell_b.reshape(1, -1), velocity)
    return binned, binned_cell.reshape(-1)


def solution(mesh):
    sizes = tuple(mesh.shape[a] for a in AXES)
    in_specs = (P(None, AXES), P(AXES), P(AXES), P(AXES), P(None, "gx", ("gy", "gz")))
    out_specs = (P(None, AXES), P(AXES))
    return jax.shard_map(
        functools.partial(shards, sizes), mesh=mesh, in_specs=in_specs, out_specs=out_specs, check_vma=False
    )
```

```python
import functools

import jax
import jax.numpy as jnp
from jax import lax
from jax.experimental import pallas as pl
from jax.experimental.pallas import tpu as pltpu
from jax.sharding import PartitionSpec as P

AXES = ("gx", "gy", "gz")
MESH = pl.DeviceIdType.MESH
F32, BF16, I32 = jnp.float32, jnp.bfloat16, jnp.int32
CAP = 256
CHUNK = 2048
LANES = 128
step_length = 0.5


def quad_weights(frac):
    return (0.5 * frac * (frac - 1.0), 1.0 - frac * frac, 0.5 * frac * (frac + 1.0))


def two_parts(x):
    high = x.astype(BF16)
    return high, (x - high.astype(F32)).astype(BF16)


def sort_phase(
    part_ref, key_ref, a_ref, b_ref,
    pos_ref, acc_ref, sorted_ref, sorted_cell_ref, table_ref, table_smem, sem, owners, between,
):
    count = part_ref.shape[1]
    chunks = count // CHUNK

    owner_ids = lax.broadcasted_iota(I32, (owners, CHUNK), 0)

    def count_chunk(i, total):
        keys = key_ref[:, pl.ds(pl.multiple_of(i * CHUNK, CHUNK), CHUNK)]
        hot = (owner_ids == keys).astype(F32)
        for j in range(CHUNK // LANES):
            total = total + hot[:, j * LANES : (j + 1) * LANES]
        return total

    spread = lax.fori_loop(0, chunks, count_chunk, jnp.zeros((owners, LANES), F32), unroll=True)
    hist = jnp.broadcast_to(jnp.sum(spread, axis=1, keepdims=True), (owners, owners))
    row = lax.broadcasted_iota(I32, (owners, owners), 0)
    col = lax.broadcasted_iota(I32, (owners, owners), 1)
    below = (col < row).astype(F32).astype(BF16)
    starts = jnp.dot(below, hist.astype(BF16), preferred_element_type=F32)
    table_ref[0:8, :] = starts.T[0:8, :].astype(I32)
    table_ref[8:16, :] = hist.T[0:8, :].astype(I32)
    copy = pltpu.make_async_copy(table_ref, table_smem, sem)
    copy.start()

    upper = (
        lax.broadcasted_iota(I32, (CAP, CAP), 0) <= lax.broadcasted_iota(I32, (CAP, CAP), 1)
    ).astype(F32).astype(BF16)
    block_ids = lax.broadcasted_iota(I32, (owners, CAP), 0)

    def rank_chunk(i, base):
        for j in range(CHUNK // CAP):
            at = pl.ds(pl.multiple_of(i * CHUNK + j * CAP, CAP), CAP)
            hot = (block_ids == key_ref[:, at]).astype(F32)
            upto = jnp.dot(hot.astype(BF16), upper, preferred_element_type=F32)
            places = jnp.sum(hot * (upto + base), axis=0, keepdims=True) - 1.0
            pos_ref[:, at] = places.astype(I32)
            base = base + upto[:, CAP - 1 : CAP]
        return base

    lax.fori_loop(0, chunks, rank_chunk, starts[:, 0:1], unroll=True)
    between()

    acc_ref[...] = jnp.zeros_like(acc_ref)
    lane_ids = lax.broadcasted_iota(I32, (CAP, CHUNK), 0)
    page_ids = lax.broadcasted_iota(I32, (32, CHUNK), 0)

    def place_chunk(i, carry):
        at = pl.ds(pl.multiple_of(i * CHUNK, CHUNK), CHUNK)
        pos = pos_ref[:, at]
        page = pos >> 8
        lane_hot = (lane_ids == (pos & 255)).astype(F32).astype(BF16)
        values = jnp.concatenate(two_parts(part_ref[:, at]), axis=0)
        page16 = jnp.broadcast_to(page, (16, CHUNK)).astype(F32).astype(BF16)
        zero = jnp.zeros((16, CHUNK), BF16)
        rows = [jnp.where(page16 == BF16(h), values, zero) for h in range(32)]
        page_hot = (page_ids == page)
        rows.append(jnp.where(page_hot, a_ref[:, at].astype(F32), 0.0).astype(BF16))
        rows.append(jnp.where(page_hot, b_ref[:, at].astype(F32), 0.0).astype(BF16))
        acc_ref[...] += lax.dot_general(
            jnp.concatenate(rows, axis=0), lane_hot, (((1,), (1,)), ((), ())),
            preferred_element_type=F32,
        )
        return carry

    lax.fori_loop(0, chunks, place_chunk, 0, unroll=True)

    cells = (acc_ref[512:544, :] * 128.0 + acc_ref[544:576, :]).astype(I32)
    for h in range(32):
        both = acc_ref[16 * h : 16 * h + 8, :] + acc_ref[16 * h + 8 : 16 * h + 16, :]
        for j in range(2):
            sorted_ref[2 * h + j] = both[:, j * LANES : (j + 1) * LANES]
            sorted_cell_ref[2 * h + j] = cells[h : h + 1, j * LANES : (j + 1) * LANES]
    for j in range(64, 67):
        sorted_ref[j] = jnp.zeros((8, LANES), F32)
        sorted_cell_ref[j] = jnp.zeros((1, LANES), I32)
    copy.wait()


def expand(d, sorted_ref, sorted_cell_ref, table_smem, send_ref, send_cell_ref):
    lanes8 = lax.broadcasted_iota(I32, (8, LANES), 1)
    lanes1 = lax.broadcasted_iota(I32, (1, LANES), 1)
    start = jnp.clip(table_smem[0, d], 0, LANES * (sorted_ref.shape[0] - 3))
    live = table_smem[8, d]
    page = start >> 7
    shift = start & 127
    turn = (LANES - shift) & 127
    head8, head1 = lanes8 < LANES - shift, lanes1 < LANES - shift
    rolled = [pltpu.roll(sorted_ref[page + j], turn, 1) for j in range(3)]
    cell_rolled = [pltpu.roll(sorted_cell_ref[page + j], turn, 1) for j in range(3)]
    for j in range(2):
        here = slice(j * LANES, (j + 1) * LANES)
        value = jnp.where(head8, rolled[j], rolled[j + 1])
        send_ref[d, :, here] = jnp.where(lanes8 < live - j * LANES, value, 0.0)
        cell = jnp.where(head1, cell_rolled[j], cell_rolled[j + 1])
        send_cell_ref[d, :, here] = jnp.where(lanes1 < live - j * LANES, cell, -1)


def prepare_field(sizes, turned_ref, rows_ref, cols_ref, field_ref, up_ref, down_ref):
    nx, ny, nz = sizes
    width, height = turned_ref.shape[1], turned_ref.shape[2]
    x = lax.axis_index("gx")
    tile = lax.axis_index("gy") * nz + lax.axis_index("gz")
    has_left, has_right = tile > 0, tile < ny * nz - 1
    left = [jnp.where(has_left, cols_ref[0, c, 7:8, :], 0.0) for c in range(2)]
    right = [jnp.where(has_right, cols_ref[1, c, 0:1, :], 0.0) for c in range(2)]
    zeros = jnp.zeros((4, height), F32)
    sides = jnp.concatenate([left[0], right[0], left[1], right[1], zeros], axis=0)
    for c, at in ((0, 0), (1, width), (None, 2 * width)):
        block = sides if c is None else turned_ref[c]
        high, low = two_parts(block)
        here = slice(at, at + block.shape[0])
        field_ref[here, 0:height] = high
        field_ref[here, height : 2 * height] = high
        field_ref[here, 2 * height : 3 * height] = low
    for ref, first, row, there in ((up_ref, 0, 7, x > 0), (down_ref, 3, 0, x < nx - 1)):
        corner = []
        for c in range(2):
            tile8 = jnp.where(there, rows_ref[first + 1, c], 0.0)
            line = tile8.T[:, row : row + 1]
            ref[c * width : (c + 1) * width, :] = jnp.broadcast_to(line, (width, LANES))
            from_left = rows_ref[first, c][row : row + 1, width - 1 : width]
            from_right = rows_ref[first + 2, c][row : row + 1, 0:1]
            corner.append(jnp.where(there & has_left, from_left, 0.0))
            corner.append(jnp.where(there & has_right, from_right, 0.0))
        corner = jnp.concatenate(corner + [jnp.zeros((4, 1), F32)], axis=0)
        ref[2 * width :, :] = jnp.broadcast_to(corner, (8, LANES))


GROUP = 8
STEP = 4
SIDE = 4


def weight_rows(data, cell, sub16, height):
    node_a = jnp.where(cell >= 0, cell >> 7, 2 * height)
    below, same, above = quad_weights(data)
    parts = [two_parts(w[0:1, :]) for w in (below, same, above)]

    def wide(v):
        return jnp.broadcast_to(v, (16, CAP))

    def wide16(v):
        return wide(v.astype(F32).astype(BF16))

    a_in, a_page = node_a & 15, node_a >> 4
    a_next = jnp.where(a_in == 15, a_page + 1, jnp.where(a_in == 0, a_page - 1, -9))
    in16, page16, next16 = wide16(a_in), wide16(a_page), wide16(a_next)
    is_below, is_same, is_above = sub16 == in16 - BF16(1), sub16 == in16, sub16 == in16 + BF16(1)
    wrap_up, wrap_down = sub16 == in16 - BF16(15), sub16 == in16 + BF16(15)
    none = jnp.zeros((16, CAP), BF16)
    near, far = [], []
    for h in range(2):
        low, mid, high = (wide(p[h]) for p in parts)
        near.append(jnp.where(is_below, low, jnp.where(is_same, mid, jnp.where(is_above, high, none))))
        far.append(jnp.where(wrap_up, high, jnp.where(wrap_down, low, none)))
    return near, far, page16, next16, none


def build_weights(data, cell, weight_ref, lanes, height):
    sub16 = lax.broadcasted_iota(I32, (16, CAP), 0).astype(F32).astype(BF16)
    near, far, page16, next16, none = weight_rows(data, cell, sub16, height)
    for c in range(height // 16):
        here_c, next_c = page16 == BF16(c), next16 == BF16(c)
        for h in range(2):
            rows = jnp.where(here_c, near[h], jnp.where(next_c, far[h], none))
            at = h * height + 16 * c
            weight_ref[at : at + 16, lanes] = rows


def mix(field_ref, weight_ref, height):
    weights = weight_ref[...]
    stacked = jnp.concatenate([weights, weights[0:height]], axis=0)
    return jnp.dot(field_ref[...], stacked, preferred_element_type=F32)


def pick_columns(data, cell, mixed_ref, up_ref, down_ref, lanes, height, width):
    sub8 = lax.broadcasted_iota(I32, (8, CAP), 0)
    node_b = cell & 127
    trio = quad_weights(data)

    def wide(v):
        return jnp.broadcast_to(v, (8, CAP))

    low, mid, high = (wide(w[1:2, :]) for w in trio)
    b_in, b_page = wide(node_b & 7), wide(node_b >> 3)
    b_next = jnp.where(b_in == 7, b_page + 1, jnp.where(b_in == 0, b_page - 1, -9))
    near = jnp.where(sub8 == b_in - 1, low, jnp.where(sub8 == b_in, mid, jnp.where(sub8 == b_in + 1, high, 0.0)))
    far = jnp.where(sub8 == b_in - 7, high, jnp.where(sub8 == b_in + 7, low, 0.0))
    first = cell < width
    edge = jnp.where(first, trio[0][0:1, :], jnp.where(cell >= (height - 1) * width, trio[2][0:1, :], 0.0))
    edge, first = wide(jnp.where(cell >= 0, edge, 0.0)), wide(cell) < width

    def rows_at(at):
        up = jnp.concatenate([up_ref[at : at + 8, :]] * 2, axis=1)
        down = jnp.concatenate([down_ref[at : at + 8, :]] * 2, axis=1)
        return mixed_ref[at : at + 8, lanes] + jnp.where(first, up, down) * edge

    picked = [[jnp.zeros((8, CAP), F32)] * 2 for _ in range(2)]
    for c in range(width // 8):
        here_c, next_c = b_page == c, b_next == c
        for k in range(2):
            block = rows_at(k * width + 8 * c)
            picked[k][0] = jnp.where(here_c, block, picked[k][0])
            picked[k][1] = jnp.where(next_c, block, picked[k][1])
    speed = []
    sides = rows_at(2 * width)
    for k in range(2):
        other = jnp.where(b_next == -1, wide(sides[2 * k : 2 * k + 1, :]), picked[k][1])
        other = jnp.where(b_next == width // 8, wide(sides[2 * k + 1 : 2 * k + 2, :]), other)
        speed.append(jnp.sum(picked[k][0] * near + other * far, axis=0, keepdims=True))
    shift = jnp.where(sub8 == 2, speed[0], jnp.where(sub8 == 3, speed[1], 0.0))
    return data + step_length * shift


def build_step(base, arrived_ref, cell_ref, weight_ref, height):
    for i in range(STEP):
        s = base + i
        here = pl.ds(pl.multiple_of(s * CAP, CAP), CAP)
        lanes = slice(i * CAP, (i + 1) * CAP)
        build_weights(arrived_ref[:, here], cell_ref[s], weight_ref, lanes, height)


def pick_step(base, arrived_ref, cell_ref, out_ref, mixed_ref, up_ref, down_ref, height, width):
    for i in range(STEP):
        s = base + i
        here = pl.ds(pl.multiple_of(s * CAP, CAP), CAP)
        lanes = slice(i * CAP, (i + 1) * CAP)
        out_ref[:, here] = pick_columns(
            arrived_ref[:, here], cell_ref[s], mixed_ref, up_ref, down_ref, lanes, height, width
        )


def wrapped(at, step, length):
    to = at + step
    return jnp.where(to >= length, to - length, to)


def rebin_kernel(
    sizes, part_in, key_in, a_in, b_in, vel_in, out_ref, cell_ref,
    part_ref, key_ref, a_ref, b_ref, vel_ref,
    pos_ref, acc_ref, sorted_ref, sorted_cell_ref, table_ref, table_smem,
    send_ref, send_cell_ref, turned_ref, rows_ref, cols_ref, field_ref, up_ref, down_ref, arrived_ref,
    weight0_ref, weight1_ref, mixed0_ref, mixed1_ref,
    load_sem, table_sem, send_sem, send_cell_sem, recv_sem, recv_cell_sem, halo_send, halo_recv,
):
    nx, ny, nz = sizes
    total = nx * ny * nz
    pairs = ((key_in, key_ref), (vel_in, vel_ref), (part_in, part_ref), (a_in, a_ref), (b_in, b_ref))
    loads = [pltpu.make_async_copy(src, dst, load_sem.at[k]) for k, (src, dst) in enumerate(pairs)]
    for load in loads:
        load.start()
    x, y, z = (lax.axis_index(a) for a in AXES)
    me = (x * ny + y) * nz + z
    tiles = ny * nz
    tile = y * nz + z
    height, width = vel_ref.shape[1], vel_ref.shape[2]
    outer, inner = y // SIDE, y % SIDE
    steps = [(0, 0), (0, 1), (1, 0), (0, 3), (3, 0), (1, 1), (3, 3), (1, 3), (3, 1), (0, 2), (2, 0), (1, 2), (2, 1), (3, 2), (2, 3), (2, 2)]
    ahead_x = [wrapped(x, d, nx) for d in range(nx)]
    ahead_y = [wrapped(outer, d, ny // SIDE) for d in range(ny // SIDE)]
    ahead_i = [wrapped(inner, d, SIDE) for d in range(SIDE)]
    ahead_z = [z, 1 - z]

    barrier = pltpu.get_barrier_semaphore()
    for a, b in steps:
        for i in range(SIDE):
            for c in range(nz):
                if (a, b, i, c) != (0, 0, 0, 0):
                    device = (ahead_x[a], ahead_y[b] * SIDE + ahead_i[i], ahead_z[c])
                    pl.semaphore_signal(barrier, inc=1, device_id=device, device_id_type=MESH)

    halos = []
    for i, dx in enumerate((1, nx - 1)):
        edge = vel_ref.at[:, pl.ds(height - 8 if dx == 1 else 0, 8), :]
        for j, dt in enumerate((1, 0, tiles - 1)):
            halos.append((edge, rows_ref.at[3 * i + j], ahead_x[dx], wrapped(tile, dt, tiles)))
    for i, dt in enumerate((1, tiles - 1)):
        edge = turned_ref.at[:, pl.ds(width - 8 if dt == 1 else 0, 8), :]
        halos.append((edge, cols_ref.at[i], x, wrapped(tile, dt, tiles)))
    halo_copies = [
        pltpu.make_async_remote_copy(
            src_ref=src, dst_ref=dst, send_sem=halo_send.at[k], recv_sem=halo_recv.at[k],
            device_id=(to_x, to_t // nz, to_t % nz), device_id_type=MESH,
        )
        for k, (src, dst, to_x, to_t) in enumerate(halos)
    ]

    def between():
        loads[1].wait()
        turned_ref[0] = vel_ref[0].T
        turned_ref[1] = vel_ref[1].T
        pl.semaphore_wait(barrier, total - 1)
        for c in halo_copies:
            c.start()
        for load in loads[2:]:
            load.wait()

    loads[0].wait()
    sort_phase(
        part_ref, key_ref, a_ref, b_ref, pos_ref, acc_ref, sorted_ref, sorted_cell_ref,
        table_ref, table_smem, table_sem, total, between,
    )

    mine = pl.ds(pl.multiple_of(me * CAP, CAP), CAP)

    def first_of(a, b):
        return (ahead_x[a] * (ny // SIDE) + ahead_y[b]) * GROUP

    def send_group(g):
        a, b = steps[g]
        for i in range(SIDE):
            for c in range(nz):
                there = first_of(a, b) + ahead_i[i] * nz + ahead_z[c]
                if (a, b, i, c) == (0, 0, 0, 0):
                    pltpu.make_async_copy(send_ref.at[there], arrived_ref.at[:, mine], recv_sem.at[g]).start()
                    pltpu.make_async_copy(send_cell_ref.at[there], cell_ref.at[me], recv_cell_sem.at[g]).start()
                    continue
                device = (ahead_x[a], ahead_y[b] * SIDE + ahead_i[i], ahead_z[c])
                pltpu.make_async_remote_copy(
                    src_ref=send_ref.at[there], dst_ref=arrived_ref.at[:, mine], send_sem=send_sem,
                    recv_sem=recv_sem.at[g], device_id=device, device_id_type=MESH,
                ).start()
                pltpu.make_async_remote_copy(
                    src_ref=send_cell_ref.at[there], dst_ref=cell_ref.at[me], send_sem=send_cell_sem,
                    recv_sem=recv_cell_sem.at[g], device_id=device, device_id_type=MESH,
                ).start()

    for g, (a, b) in enumerate(steps):
        base = first_of(a, b)

        def expand_one(i, carry, base=base):
            expand(base + i, sorted_ref, sorted_cell_ref, table_smem, send_ref, send_cell_ref)
            return carry

        lax.fori_loop(0, GROUP, expand_one, 0, unroll=True)
        if g > 0:
            send_group(g - 1)
    groups = len(steps)
    send_group(groups - 1)

    for c in halo_copies:
        c.wait()
    prepare_field(sizes, turned_ref, rows_ref, cols_ref, field_ref, up_ref, down_ref)

    def source_base(g):
        shift = jnp.int32(2) * g
        step_x = lax.shift_right_arithmetic(jnp.int32(-1369213168), shift) & 3
        step_y = lax.shift_right_arithmetic(jnp.int32(-1182141244), shift) & 3
        back_x = (x + nx - step_x) % nx
        back_y = (outer + ny // SIDE - step_y) % (ny // SIDE)
        return (back_x * (ny // SIDE) + back_y) * GROUP

    def arrive(g):
        blocks = arrived_ref.at[:, pl.ds(0, GROUP * CAP)]
        pltpu.make_async_copy(blocks, blocks, recv_sem.at[g]).wait()
        few = cell_ref.at[pl.ds(0, GROUP)]
        pltpu.make_async_copy(few, few, recv_cell_sem.at[g]).wait()

    build = lambda base, ref: build_step(base, arrived_ref, cell_ref, ref, height)
    pick = lambda base, ref: pick_step(
        base, arrived_ref, cell_ref, out_ref, ref, up_ref, down_ref, height, width
    )
    arrive(0)
    start = source_base(0)
    build(start, weight0_ref)
    mixed0_ref[...] = mix(field_ref, weight0_ref, height)
    build(start + STEP, weight1_ref)

    def one_group(g, before):
        arrive(g)
        base = source_base(g)
        mixed1_ref[...] = mix(field_ref, weight1_ref, height)
        pick(before, mixed0_ref)
        build(base, weight0_ref)
        mixed0_ref[...] = mix(field_ref, weight0_ref, height)
        pick(before + STEP, mixed1_ref)
        build(base + STEP, weight1_ref)
        return base

    last = lax.fori_loop(1, groups, one_group, start)
    mixed1_ref[...] = mix(field_ref, weight1_ref, height)
    pick(last, mixed0_ref)
    pick(last + STEP, mixed1_ref)
    some = send_ref.at[pl.ds(0, total - 1)]
    some_cell = send_cell_ref.at[pl.ds(0, total - 1)]
    pltpu.make_async_copy(some, some, send_sem).wait()
    pltpu.make_async_copy(some_cell, some_cell, send_cell_sem).wait()


def shards(sizes, particles, dest_key, cell_a, cell_b, velocity):
    owners = sizes[0] * sizes[1] * sizes[2]
    count = particles.shape[1]
    parts, height, width = velocity.shape
    vmem = pl.BlockSpec(memory_space=pltpu.VMEM)
    dma = pltpu.SemaphoreType.DMA
    groups = owners // GROUP
    binned, binned_cell = pl.pallas_call(
        functools.partial(rebin_kernel, sizes),
        out_shape=(
            pltpu.VMEM((8, owners * CAP), F32),
            pltpu.VMEM((owners, 1, CAP), I32),
        ),
        in_specs=[pl.BlockSpec(memory_space=pltpu.HBM)] * 5,
        out_specs=(vmem,) * 2,
        scratch_shapes=[
            pltpu.VMEM(particles.shape, F32),
            pltpu.VMEM((1, count), I32),
            pltpu.VMEM((1, count), I32),
            pltpu.VMEM((1, count), I32),
            pltpu.VMEM(velocity.shape, F32),
            pltpu.VMEM((1, count), I32),
            pltpu.VMEM((576, CAP), F32),
            pltpu.VMEM((67, 8, LANES), F32),
            pltpu.VMEM((67, 1, LANES), I32),
            pltpu.VMEM((16, LANES), I32),
            pltpu.SMEM((16, LANES), I32),
            pltpu.VMEM((owners, 8, CAP), F32),
            pltpu.VMEM((owners, 1, CAP), I32),
            pltpu.VMEM((parts, width, height), F32),
            pltpu.VMEM((6, parts, 8, width), F32),
            pltpu.VMEM((2, parts, 8, height), F32),
            pltpu.VMEM((2 * width + 8, 3 * height), BF16),
            pltpu.VMEM((2 * width + 8, LANES), F32),
            pltpu.VMEM((2 * width + 8, LANES), F32),
            pltpu.VMEM((8, owners * CAP), F32),
            pltpu.VMEM((2 * height, STEP * CAP), BF16),
            pltpu.VMEM((2 * height, STEP * CAP), BF16),
            pltpu.VMEM((2 * width + 8, STEP * CAP), F32),
            pltpu.VMEM((2 * width + 8, STEP * CAP), F32),
            dma((5,)), dma, dma, dma, dma((groups,)), dma((groups,)), dma((8,)), dma((8,)),
        ],
        compiler_params=pltpu.CompilerParams(collective_id=0, has_side_effects=True),
        name="rebin",
    )(particles, dest_key.reshape(1, -1), cell_a.reshape(1, -1), cell_b.reshape(1, -1), velocity)
    return binned, binned_cell.reshape(-1)


def solution(mesh):
    sizes = tuple(mesh.shape[a] for a in AXES)
    in_specs = (P(None, AXES), P(AXES), P(AXES), P(AXES), P(None, "gx", ("gy", "gz")))
    out_specs = (P(None, AXES), P(AXES))
    return jax.shard_map(
        functools.partial(shards, sizes), mesh=mesh, in_specs=in_specs, out_specs=out_specs, check_vma=False
    )
```

```python
import functools

import jax
import jax.numpy as jnp
from jax import lax
from jax.experimental import pallas as pl
from jax.experimental.pallas import tpu as pltpu
from jax.sharding import PartitionSpec as P

AXES = ("gx", "gy", "gz")
MESH = pl.DeviceIdType.MESH
F32, BF16, I32 = jnp.float32, jnp.bfloat16, jnp.int32
CAP = 256
CHUNK = 2048
LANES = 128
step_length = 0.5


def quad_weights(frac):
    return (0.5 * frac * (frac - 1.0), 1.0 - frac * frac, 0.5 * frac * (frac + 1.0))


def two_parts(x):
    high = x.astype(BF16)
    return high, (x - high.astype(F32)).astype(BF16)


def sort_phase(
    part_ref, key_ref, a_ref, b_ref,
    pos_ref, acc_ref, sorted_ref, sorted_cell_ref, table_ref, table_smem, sem, owners, between,
):
    count = part_ref.shape[1]
    chunks = count // CHUNK

    owner_ids = lax.broadcasted_iota(I32, (owners, CHUNK), 0)

    def count_chunk(i, total):
        keys = key_ref[:, pl.ds(pl.multiple_of(i * CHUNK, CHUNK), CHUNK)]
        hot = (owner_ids == keys).astype(F32)
        for j in range(CHUNK // LANES):
            total = total + hot[:, j * LANES : (j + 1) * LANES]
        return total

    spread = lax.fori_loop(0, chunks, count_chunk, jnp.zeros((owners, LANES), F32), unroll=True)
    hist = jnp.broadcast_to(jnp.sum(spread, axis=1, keepdims=True), (owners, owners))
    row = lax.broadcasted_iota(I32, (owners, owners), 0)
    col = lax.broadcasted_iota(I32, (owners, owners), 1)
    below = (col < row).astype(F32).astype(BF16)
    starts = jnp.dot(below, hist.astype(BF16), preferred_element_type=F32)
    table_ref[0:8, :] = starts.T[0:8, :].astype(I32)
    table_ref[8:16, :] = hist.T[0:8, :].astype(I32)
    copy = pltpu.make_async_copy(table_ref, table_smem, sem)
    copy.start()

    upper = (
        lax.broadcasted_iota(I32, (CAP, CAP), 0) <= lax.broadcasted_iota(I32, (CAP, CAP), 1)
    ).astype(F32).astype(BF16)
    block_ids = lax.broadcasted_iota(I32, (owners, CAP), 0)

    def rank_chunk(i, base):
        for j in range(CHUNK // CAP):
            at = pl.ds(pl.multiple_of(i * CHUNK + j * CAP, CAP), CAP)
            hot = (block_ids == key_ref[:, at]).astype(F32)
            upto = jnp.dot(hot.astype(BF16), upper, preferred_element_type=F32)
            places = jnp.sum(hot * (upto + base), axis=0, keepdims=True) - 1.0
            pos_ref[:, at] = places.astype(I32)
            base = base + upto[:, CAP - 1 : CAP]
        return base

    lax.fori_loop(0, chunks, rank_chunk, starts[:, 0:1], unroll=True)
    between()

    acc_ref[...] = jnp.zeros_like(acc_ref)
    lane_ids = lax.broadcasted_iota(I32, (CAP, CHUNK), 0)
    page_ids = lax.broadcasted_iota(I32, (32, CHUNK), 0)

    def place_chunk(i, carry):
        at = pl.ds(pl.multiple_of(i * CHUNK, CHUNK), CHUNK)
        pos = pos_ref[:, at]
        page = pos >> 8
        lane_hot = (lane_ids == (pos & 255)).astype(F32).astype(BF16)
        values = jnp.concatenate(two_parts(part_ref[:, at]), axis=0)
        page16 = jnp.broadcast_to(page, (16, CHUNK)).astype(F32).astype(BF16)
        zero = jnp.zeros((16, CHUNK), BF16)
        rows = [jnp.where(page16 == BF16(h), values, zero) for h in range(32)]
        page_hot = (page_ids == page)
        rows.append(jnp.where(page_hot, a_ref[:, at].astype(F32), 0.0).astype(BF16))
        rows.append(jnp.where(page_hot, b_ref[:, at].astype(F32), 0.0).astype(BF16))
        acc_ref[...] += lax.dot_general(
            jnp.concatenate(rows, axis=0), lane_hot, (((1,), (1,)), ((), ())),
            preferred_element_type=F32,
        )
        return carry

    lax.fori_loop(0, chunks, place_chunk, 0, unroll=True)

    cells = (acc_ref[512:544, :] * 128.0 + acc_ref[544:576, :]).astype(I32)
    for h in range(32):
        both = acc_ref[16 * h : 16 * h + 8, :] + acc_ref[16 * h + 8 : 16 * h + 16, :]
        for j in range(2):
            sorted_ref[2 * h + j] = both[:, j * LANES : (j + 1) * LANES]
            sorted_cell_ref[2 * h + j] = cells[h : h + 1, j * LANES : (j + 1) * LANES]
    for j in range(64, 67):
        sorted_ref[j] = jnp.zeros((8, LANES), F32)
        sorted_cell_ref[j] = jnp.zeros((1, LANES), I32)
    copy.wait()


def expand(d, sorted_ref, sorted_cell_ref, table_smem, send_ref, send_cell_ref):
    lanes8 = lax.broadcasted_iota(I32, (8, LANES), 1)
    lanes1 = lax.broadcasted_iota(I32, (1, LANES), 1)
    start = jnp.clip(table_smem[0, d], 0, LANES * (sorted_ref.shape[0] - 3))
    live = table_smem[8, d]
    page = start >> 7
    shift = start & 127
    turn = (LANES - shift) & 127
    head8, head1 = lanes8 < LANES - shift, lanes1 < LANES - shift
    rolled = [pltpu.roll(sorted_ref[page + j], turn, 1) for j in range(3)]
    cell_rolled = [pltpu.roll(sorted_cell_ref[page + j], turn, 1) for j in range(3)]
    for j in range(2):
        here = slice(j * LANES, (j + 1) * LANES)
        value = jnp.where(head8, rolled[j], rolled[j + 1])
        send_ref[d, :, here] = jnp.where(lanes8 < live - j * LANES, value, 0.0)
        cell = jnp.where(head1, cell_rolled[j], cell_rolled[j + 1])
        send_cell_ref[d, :, here] = jnp.where(lanes1 < live - j * LANES, cell, -1)


def prepare_field(sizes, turned_ref, rows_ref, cols_ref, field_ref, up_ref, down_ref):
    nx, ny, nz = sizes
    width, height = turned_ref.shape[1], turned_ref.shape[2]
    x = lax.axis_index("gx")
    tile = lax.axis_index("gy") * nz + lax.axis_index("gz")
    has_left, has_right = tile > 0, tile < ny * nz - 1
    left = [jnp.where(has_left, cols_ref[0, c, 7:8, :], 0.0) for c in range(2)]
    right = [jnp.where(has_right, cols_ref[1, c, 0:1, :], 0.0) for c in range(2)]
    zeros = jnp.zeros((4, height), F32)
    sides = jnp.concatenate([left[0], right[0], left[1], right[1], zeros], axis=0)
    for c, at in ((0, 0), (1, width), (None, 2 * width)):
        block = sides if c is None else turned_ref[c]
        high, low = two_parts(block)
        here = slice(at, at + block.shape[0])
        field_ref[here, 0:height] = high
        field_ref[here, height : 2 * height] = high
        field_ref[here, 2 * height : 3 * height] = low
    for ref, first, row, there in ((up_ref, 0, 7, x > 0), (down_ref, 3, 0, x < nx - 1)):
        corner = []
        for c in range(2):
            tile8 = jnp.where(there, rows_ref[first + 1, c], 0.0)
            line = tile8.T[:, row : row + 1]
            ref[c * width : (c + 1) * width, :] = jnp.broadcast_to(line, (width, LANES))
            from_left = rows_ref[first, c][row : row + 1, width - 1 : width]
            from_right = rows_ref[first + 2, c][row : row + 1, 0:1]
            corner.append(jnp.where(there & has_left, from_left, 0.0))
            corner.append(jnp.where(there & has_right, from_right, 0.0))
        corner = jnp.concatenate(corner + [jnp.zeros((4, 1), F32)], axis=0)
        ref[2 * width :, :] = jnp.broadcast_to(corner, (8, LANES))


GROUP = 8
STEP = 4
SIDE = 4


def weight_rows(data, cell, sub16, height):
    node_a = jnp.where(cell >= 0, cell >> 7, 2 * height)
    below, same, above = quad_weights(data)
    parts = [two_parts(w[0:1, :]) for w in (below, same, above)]

    def wide(v):
        return jnp.broadcast_to(v, (16, CAP))

    def wide16(v):
        return wide(v.astype(F32).astype(BF16))

    a_in, a_page = node_a & 15, node_a >> 4
    a_next = jnp.where(a_in == 15, a_page + 1, jnp.where(a_in == 0, a_page - 1, -9))
    in16, page16, next16 = wide16(a_in), wide16(a_page), wide16(a_next)
    is_below, is_same, is_above = sub16 == in16 - BF16(1), sub16 == in16, sub16 == in16 + BF16(1)
    wrap_up, wrap_down = sub16 == in16 - BF16(15), sub16 == in16 + BF16(15)
    none = jnp.zeros((16, CAP), BF16)
    near, far = [], []
    for h in range(2):
        low, mid, high = (wide(p[h]) for p in parts)
        near.append(jnp.where(is_below, low, jnp.where(is_same, mid, jnp.where(is_above, high, none))))
        far.append(jnp.where(wrap_up, high, jnp.where(wrap_down, low, none)))
    return near, far, page16, next16, none


def build_weights(data, cell, weight_ref, lanes, height):
    sub16 = lax.broadcasted_iota(I32, (16, CAP), 0).astype(F32).astype(BF16)
    near, far, page16, next16, none = weight_rows(data, cell, sub16, height)
    for c in range(height // 16):
        here_c, next_c = page16 == BF16(c), next16 == BF16(c)
        for h in range(2):
            rows = jnp.where(here_c, near[h], jnp.where(next_c, far[h], none))
            at = h * height + 16 * c
            weight_ref[at : at + 16, lanes] = rows


def mix(field_ref, weight_ref, height):
    weights = weight_ref[...]
    stacked = jnp.concatenate([weights, weights[0:height]], axis=0)
    return jnp.dot(field_ref[...], stacked, preferred_element_type=F32)


def pick_columns(data, cell, mixed_ref, up_ref, down_ref, lanes, height, width):
    sub8 = lax.broadcasted_iota(I32, (8, CAP), 0)
    node_b = cell & 127
    trio = quad_weights(data)

    def wide(v):
        return jnp.broadcast_to(v, (8, CAP))

    low, mid, high = (wide(w[1:2, :]) for w in trio)
    b_in, b_page = wide(node_b & 7), wide(node_b >> 3)
    b_next = jnp.where(b_in == 7, b_page + 1, jnp.where(b_in == 0, b_page - 1, -9))
    near = jnp.where(sub8 == b_in - 1, low, jnp.where(sub8 == b_in, mid, jnp.where(sub8 == b_in + 1, high, 0.0)))
    far = jnp.where(sub8 == b_in - 7, high, jnp.where(sub8 == b_in + 7, low, 0.0))
    first = cell < width
    edge = jnp.where(first, trio[0][0:1, :], jnp.where(cell >= (height - 1) * width, trio[2][0:1, :], 0.0))
    edge, first = wide(jnp.where(cell >= 0, edge, 0.0)), wide(cell) < width

    def rows_at(at):
        up = jnp.concatenate([up_ref[at : at + 8, :]] * 2, axis=1)
        down = jnp.concatenate([down_ref[at : at + 8, :]] * 2, axis=1)
        return mixed_ref[at : at + 8, lanes] + jnp.where(first, up, down) * edge

    picked = [[jnp.zeros((8, CAP), F32)] * 2 for _ in range(2)]
    for c in range(width // 8):
        here_c, next_c = b_page == c, b_next == c
        for k in range(2):
            block = rows_at(k * width + 8 * c)
            picked[k][0] = jnp.where(here_c, block, picked[k][0])
            picked[k][1] = jnp.where(next_c, block, picked[k][1])
    speed = []
    sides = rows_at(2 * width)
    for k in range(2):
        other = jnp.where(b_next == -1, wide(sides[2 * k : 2 * k + 1, :]), picked[k][1])
        other = jnp.where(b_next == width // 8, wide(sides[2 * k + 1 : 2 * k + 2, :]), other)
        speed.append(jnp.sum(picked[k][0] * near + other * far, axis=0, keepdims=True))
    shift = jnp.where(sub8 == 2, speed[0], jnp.where(sub8 == 3, speed[1], 0.0))
    return data + step_length * shift


def build_step(base, arrived_ref, cell_ref, weight_ref, height):
    for i in range(STEP):
        s = base + i
        here = pl.ds(pl.multiple_of(s * CAP, CAP), CAP)
        lanes = slice(i * CAP, (i + 1) * CAP)
        build_weights(arrived_ref[:, here], cell_ref[s], weight_ref, lanes, height)


def pick_step(base, arrived_ref, cell_ref, out_ref, mixed_ref, up_ref, down_ref, height, width):
    for i in range(STEP):
        s = base + i
        here = pl.ds(pl.multiple_of(s * CAP, CAP), CAP)
        lanes = slice(i * CAP, (i + 1) * CAP)
        out_ref[:, here] = pick_columns(
            arrived_ref[:, here], cell_ref[s], mixed_ref, up_ref, down_ref, lanes, height, width
        )


def wrapped(at, step, length):
    to = at + step
    return jnp.where(to >= length, to - length, to)


def rebin_kernel(
    sizes, part_in, key_in, a_in, b_in, vel_in, out_ref, cell_ref,
    part_ref, key_ref, a_ref, b_ref, vel_ref,
    pos_ref, acc_ref, sorted_ref, sorted_cell_ref, table_ref, table_smem,
    send_ref, send_cell_ref, turned_ref, rows_ref, cols_ref, field_ref, up_ref, down_ref, arrived_ref,
    weight0_ref, weight1_ref, mixed0_ref, mixed1_ref,
    load_sem, table_sem, send_sem, send_cell_sem, recv_sem, recv_cell_sem, halo_send, halo_recv,
):
    nx, ny, nz = sizes
    total = nx * ny * nz
    pairs = ((key_in, key_ref), (vel_in, vel_ref), (part_in, part_ref), (a_in, a_ref), (b_in, b_ref))
    loads = [pltpu.make_async_copy(src, dst, load_sem.at[k]) for k, (src, dst) in enumerate(pairs)]
    for load in loads:
        load.start()
    x, y, z = (lax.axis_index(a) for a in AXES)
    me = (x * ny + y) * nz + z
    tiles = ny * nz
    tile = y * nz + z
    height, width = vel_ref.shape[1], vel_ref.shape[2]
    outer, inner = y // SIDE, y % SIDE
    steps = [(0, 0), (0, 1), (1, 0), (0, 3), (3, 0), (1, 1), (3, 3), (1, 3), (3, 1), (0, 2), (2, 0), (1, 2), (2, 1), (3, 2), (2, 3), (2, 2)]
    ahead_x = [wrapped(x, d, nx) for d in range(nx)]
    ahead_y = [wrapped(outer, d, ny // SIDE) for d in range(ny // SIDE)]
    ahead_i = [wrapped(inner, d, SIDE) for d in range(SIDE)]
    ahead_z = [z, 1 - z]

    barrier = pltpu.get_barrier_semaphore()
    for a, b in steps:
        for i in range(SIDE):
            for c in range(nz):
                if (a, b, i, c) != (0, 0, 0, 0):
                    device = (ahead_x[a], ahead_y[b] * SIDE + ahead_i[i], ahead_z[c])
                    pl.semaphore_signal(barrier, inc=1, device_id=device, device_id_type=MESH)

    halos = []
    for i, dx in enumerate((1, nx - 1)):
        edge = vel_ref.at[:, pl.ds(height - 8 if dx == 1 else 0, 8), :]
        for j, dt in enumerate((1, 0, tiles - 1)):
            halos.append((edge, rows_ref.at[3 * i + j], ahead_x[dx], wrapped(tile, dt, tiles)))
    for i, dt in enumerate((1, tiles - 1)):
        edge = turned_ref.at[:, pl.ds(width - 8 if dt == 1 else 0, 8), :]
        halos.append((edge, cols_ref.at[i], x, wrapped(tile, dt, tiles)))
    halo_copies = [
        pltpu.make_async_remote_copy(
            src_ref=src, dst_ref=dst, send_sem=halo_send.at[k], recv_sem=halo_recv.at[k],
            device_id=(to_x, to_t // nz, to_t % nz), device_id_type=MESH,
        )
        for k, (src, dst, to_x, to_t) in enumerate(halos)
    ]

    def between():
        loads[1].wait()
        turned_ref[0] = vel_ref[0].T
        turned_ref[1] = vel_ref[1].T
        for load in loads[2:]:
            load.wait()

    loads[0].wait()
    sort_phase(
        part_ref, key_ref, a_ref, b_ref, pos_ref, acc_ref, sorted_ref, sorted_cell_ref,
        table_ref, table_smem, table_sem, total, between,
    )
    pl.semaphore_wait(barrier, total - 1)
    for c in halo_copies:
        c.start()

    mine = pl.ds(pl.multiple_of(me * CAP, CAP), CAP)

    def first_of(a, b):
        return (ahead_x[a] * (ny // SIDE) + ahead_y[b]) * GROUP

    def send_group(g):
        a, b = steps[g]
        for i in range(SIDE):
            for c in range(nz):
                there = first_of(a, b) + ahead_i[i] * nz + ahead_z[c]
                if (a, b, i, c) == (0, 0, 0, 0):
                    pltpu.make_async_copy(send_ref.at[there], arrived_ref.at[:, mine], recv_sem.at[g]).start()
                    pltpu.make_async_copy(send_cell_ref.at[there], cell_ref.at[me], recv_cell_sem.at[g]).start()
                    continue
                device = (ahead_x[a], ahead_y[b] * SIDE + ahead_i[i], ahead_z[c])
                pltpu.make_async_remote_copy(
                    src_ref=send_ref.at[there], dst_ref=arrived_ref.at[:, mine], send_sem=send_sem,
                    recv_sem=recv_sem.at[g], device_id=device, device_id_type=MESH,
                ).start()
                pltpu.make_async_remote_copy(
                    src_ref=send_cell_ref.at[there], dst_ref=cell_ref.at[me], send_sem=send_cell_sem,
                    recv_sem=recv_cell_sem.at[g], device_id=device, device_id_type=MESH,
                ).start()

    for g, (a, b) in enumerate(steps):
        base = first_of(a, b)

        def expand_one(i, carry, base=base):
            expand(base + i, sorted_ref, sorted_cell_ref, table_smem, send_ref, send_cell_ref)
            return carry

        lax.fori_loop(0, GROUP, expand_one, 0, unroll=True)
        if g > 0:
            send_group(g - 1)
    groups = len(steps)
    send_group(groups - 1)

    for c in halo_copies:
        c.wait()
    prepare_field(sizes, turned_ref, rows_ref, cols_ref, field_ref, up_ref, down_ref)

    def source_base(g):
        shift = jnp.int32(2) * g
        step_x = lax.shift_right_arithmetic(jnp.int32(-1369213168), shift) & 3
        step_y = lax.shift_right_arithmetic(jnp.int32(-1182141244), shift) & 3
        back_x = (x + nx - step_x) % nx
        back_y = (outer + ny // SIDE - step_y) % (ny // SIDE)
        return (back_x * (ny // SIDE) + back_y) * GROUP

    def arrive(g):
        blocks = arrived_ref.at[:, pl.ds(0, GROUP * CAP)]
        pltpu.make_async_copy(blocks, blocks, recv_sem.at[g]).wait()
        few = cell_ref.at[pl.ds(0, GROUP)]
        pltpu.make_async_copy(few, few, recv_cell_sem.at[g]).wait()

    build = lambda base, ref: build_step(base, arrived_ref, cell_ref, ref, height)
    pick = lambda base, ref: pick_step(
        base, arrived_ref, cell_ref, out_ref, ref, up_ref, down_ref, height, width
    )
    arrive(0)
    start = source_base(0)
    build(start, weight0_ref)
    mixed0_ref[...] = mix(field_ref, weight0_ref, height)
    build(start + STEP, weight1_ref)

    def one_group(g, before):
        arrive(g)
        base = source_base(g)
        mixed1_ref[...] = mix(field_ref, weight1_ref, height)
        pick(before, mixed0_ref)
        build(base, weight0_ref)
        mixed0_ref[...] = mix(field_ref, weight0_ref, height)
        pick(before + STEP, mixed1_ref)
        build(base + STEP, weight1_ref)
        return base

    last = lax.fori_loop(1, groups, one_group, start)
    mixed1_ref[...] = mix(field_ref, weight1_ref, height)
    pick(last, mixed0_ref)
    pick(last + STEP, mixed1_ref)
    some = send_ref.at[pl.ds(0, total - 1)]
    some_cell = send_cell_ref.at[pl.ds(0, total - 1)]
    pltpu.make_async_copy(some, some, send_sem).wait()
    pltpu.make_async_copy(some_cell, some_cell, send_cell_sem).wait()


def shards(sizes, particles, dest_key, cell_a, cell_b, velocity):
    owners = sizes[0] * sizes[1] * sizes[2]
    count = particles.shape[1]
    parts, height, width = velocity.shape
    vmem = pl.BlockSpec(memory_space=pltpu.VMEM)
    dma = pltpu.SemaphoreType.DMA
    groups = owners // GROUP
    binned, binned_cell = pl.pallas_call(
        functools.partial(rebin_kernel, sizes),
        out_shape=(
            pltpu.VMEM((8, owners * CAP), F32),
            pltpu.VMEM((owners, 1, CAP), I32),
        ),
        in_specs=[pl.BlockSpec(memory_space=pltpu.HBM)] * 5,
        out_specs=(vmem,) * 2,
        scratch_shapes=[
            pltpu.VMEM(particles.shape, F32),
            pltpu.VMEM((1, count), I32),
            pltpu.VMEM((1, count), I32),
            pltpu.VMEM((1, count), I32),
            pltpu.VMEM(velocity.shape, F32),
            pltpu.VMEM((1, count), I32),
            pltpu.VMEM((576, CAP), F32),
            pltpu.VMEM((67, 8, LANES), F32),
            pltpu.VMEM((67, 1, LANES), I32),
            pltpu.VMEM((16, LANES), I32),
            pltpu.SMEM((16, LANES), I32),
            pltpu.VMEM((owners, 8, CAP), F32),
            pltpu.VMEM((owners, 1, CAP), I32),
            pltpu.VMEM((parts, width, height), F32),
            pltpu.VMEM((6, parts, 8, width), F32),
            pltpu.VMEM((2, parts, 8, height), F32),
            pltpu.VMEM((2 * width + 8, 3 * height), BF16),
            pltpu.VMEM((2 * width + 8, LANES), F32),
            pltpu.VMEM((2 * width + 8, LANES), F32),
            pltpu.VMEM((8, owners * CAP), F32),
            pltpu.VMEM((2 * height, STEP * CAP), BF16),
            pltpu.VMEM((2 * height, STEP * CAP), BF16),
            pltpu.VMEM((2 * width + 8, STEP * CAP), F32),
            pltpu.VMEM((2 * width + 8, STEP * CAP), F32),
            dma((5,)), dma, dma, dma, dma((groups,)), dma((groups,)), dma((8,)), dma((8,)),
        ],
        compiler_params=pltpu.CompilerParams(collective_id=0, has_side_effects=True),
        name="rebin",
    )(particles, dest_key.reshape(1, -1), cell_a.reshape(1, -1), cell_b.reshape(1, -1), velocity)
    return binned, binned_cell.reshape(-1)


def solution(mesh):
    sizes = tuple(mesh.shape[a] for a in AXES)
    in_specs = (P(None, AXES), P(AXES), P(AXES), P(AXES), P(None, "gx", ("gy", "gz")))
    out_specs = (P(None, AXES), P(AXES))
    return jax.shard_map(
        functools.partial(shards, sizes), mesh=mesh, in_specs=in_specs, out_specs=out_specs, check_vma=False
    )
```

```python
import functools

import jax
import jax.numpy as jnp
from jax import lax
from jax.experimental import pallas as pl
from jax.experimental.pallas import tpu as pltpu
from jax.sharding import PartitionSpec as P

AXES = ("gx", "gy", "gz")
MESH = pl.DeviceIdType.MESH
F32, BF16, I32 = jnp.float32, jnp.bfloat16, jnp.int32
CAP = 256
CHUNK = 2048
LANES = 128
step_length = 0.5


def quad_weights(frac):
    return (0.5 * frac * (frac - 1.0), 1.0 - frac * frac, 0.5 * frac * (frac + 1.0))


def two_parts(x):
    high = x.astype(BF16)
    return high, (x - high.astype(F32)).astype(BF16)


def sort_phase(
    part_ref, key_ref, a_ref, b_ref,
    pos_ref, acc_ref, sorted_ref, sorted_cell_ref, table_ref, table_smem, sem, owners, between,
):
    count = part_ref.shape[1]
    chunks = count // CHUNK

    owner_ids = lax.broadcasted_iota(I32, (owners, CHUNK), 0)

    def count_chunk(i, total):
        keys = key_ref[:, pl.ds(pl.multiple_of(i * CHUNK, CHUNK), CHUNK)]
        hot = (owner_ids == keys).astype(F32)
        for j in range(CHUNK // LANES):
            total = total + hot[:, j * LANES : (j + 1) * LANES]
        return total

    spread = lax.fori_loop(0, chunks, count_chunk, jnp.zeros((owners, LANES), F32), unroll=True)
    hist = jnp.broadcast_to(jnp.sum(spread, axis=1, keepdims=True), (owners, owners))
    row = lax.broadcasted_iota(I32, (owners, owners), 0)
    col = lax.broadcasted_iota(I32, (owners, owners), 1)
    below = (col < row).astype(F32).astype(BF16)
    starts = jnp.dot(below, hist.astype(BF16), preferred_element_type=F32)
    table_ref[0:8, :] = starts.T[0:8, :].astype(I32)
    table_ref[8:16, :] = hist.T[0:8, :].astype(I32)
    copy = pltpu.make_async_copy(table_ref, table_smem, sem)
    copy.start()

    upper = (
        lax.broadcasted_iota(I32, (CAP, CAP), 0) <= lax.broadcasted_iota(I32, (CAP, CAP), 1)
    ).astype(F32).astype(BF16)
    block_ids = lax.broadcasted_iota(I32, (owners, CAP), 0)

    def rank_chunk(i, base):
        for j in range(CHUNK // CAP):
            at = pl.ds(pl.multiple_of(i * CHUNK + j * CAP, CAP), CAP)
            hot = (block_ids == key_ref[:, at]).astype(F32)
            upto = jnp.dot(hot.astype(BF16), upper, preferred_element_type=F32)
            places = jnp.sum(hot * (upto + base), axis=0, keepdims=True) - 1.0
            pos_ref[:, at] = places.astype(I32)
            base = base + upto[:, CAP - 1 : CAP]
        return base

    lax.fori_loop(0, chunks, rank_chunk, starts[:, 0:1], unroll=True)
    between()

    lane_ids = lax.broadcasted_iota(I32, (CAP, CHUNK), 0)
    page_ids = lax.broadcasted_iota(I32, (32, CHUNK), 0)

    def place_chunk(i):
        at = pl.ds(i * CHUNK, CHUNK)
        pos = pos_ref[:, at]
        page = pos >> 8
        lane_hot = (lane_ids == (pos & 255)).astype(F32).astype(BF16)
        values = jnp.concatenate(two_parts(part_ref[:, at]), axis=0)
        page16 = jnp.broadcast_to(page, (16, CHUNK)).astype(F32).astype(BF16)
        zero = jnp.zeros((16, CHUNK), BF16)
        rows = [jnp.where(page16 == BF16(h), values, zero) for h in range(32)]
        page_hot = (page_ids == page)
        rows.append(jnp.where(page_hot, a_ref[:, at].astype(F32), 0.0).astype(BF16))
        rows.append(jnp.where(page_hot, b_ref[:, at].astype(F32), 0.0).astype(BF16))
        return lax.dot_general(
            jnp.concatenate(rows, axis=0), lane_hot, (((1,), (1,)), ((), ())),
            preferred_element_type=F32,
        )

    acc_ref[...] = place_chunk(0)
    for i in range(1, chunks):
        acc_ref[...] += place_chunk(i)

    cells = (acc_ref[512:544, :] * 128.0 + acc_ref[544:576, :]).astype(I32)
    for h in range(32):
        both = acc_ref[16 * h : 16 * h + 8, :] + acc_ref[16 * h + 8 : 16 * h + 16, :]
        for j in range(2):
            sorted_ref[2 * h + j] = both[:, j * LANES : (j + 1) * LANES]
            sorted_cell_ref[2 * h + j] = cells[h : h + 1, j * LANES : (j + 1) * LANES]
    for j in range(64, 67):
        sorted_ref[j] = jnp.zeros((8, LANES), F32)
        sorted_cell_ref[j] = jnp.zeros((1, LANES), I32)
    copy.wait()


def expand(d, sorted_ref, sorted_cell_ref, table_smem, send_ref, send_cell_ref):
    lanes8 = lax.broadcasted_iota(I32, (8, LANES), 1)
    lanes1 = lax.broadcasted_iota(I32, (1, LANES), 1)
    start = jnp.clip(table_smem[0, d], 0, LANES * (sorted_ref.shape[0] - 3))
    live = table_smem[8, d]
    page = start >> 7
    shift = start & 127
    turn = (LANES - shift) & 127
    head8, head1 = lanes8 < LANES - shift, lanes1 < LANES - shift
    rolled = [pltpu.roll(sorted_ref[page + j], turn, 1) for j in range(3)]
    cell_rolled = [pltpu.roll(sorted_cell_ref[page + j], turn, 1) for j in range(3)]
    for j in range(2):
        here = slice(j * LANES, (j + 1) * LANES)
        value = jnp.where(head8, rolled[j], rolled[j + 1])
        send_ref[d, :, here] = jnp.where(lanes8 < live - j * LANES, value, 0.0)
        cell = jnp.where(head1, cell_rolled[j], cell_rolled[j + 1])
        send_cell_ref[d, :, here] = jnp.where(lanes1 < live - j * LANES, cell, -1)


def prepare_field(sizes, turned_ref, rows_ref, cols_ref, field_ref, up_ref, down_ref):
    nx, ny, nz = sizes
    width, height = turned_ref.shape[1], turned_ref.shape[2]
    x = lax.axis_index("gx")
    tile = lax.axis_index("gy") * nz + lax.axis_index("gz")
    has_left, has_right = tile > 0, tile < ny * nz - 1
    left = [jnp.where(has_left, cols_ref[0, c, 7:8, :], 0.0) for c in range(2)]
    right = [jnp.where(has_right, cols_ref[1, c, 0:1, :], 0.0) for c in range(2)]
    zeros = jnp.zeros((4, height), F32)
    sides = jnp.concatenate([left[0], right[0], left[1], right[1], zeros], axis=0)
    for c, at in ((0, 0), (1, width), (None, 2 * width)):
        block = sides if c is None else turned_ref[c]
        high, low = two_parts(block)
        here = slice(at, at + block.shape[0])
        field_ref[here, 0:height] = high
        field_ref[here, height : 2 * height] = high
        field_ref[here, 2 * height : 3 * height] = low
    for ref, first, row, there in ((up_ref, 0, 7, x > 0), (down_ref, 3, 0, x < nx - 1)):
        corner = []
        for c in range(2):
            tile8 = jnp.where(there, rows_ref[first + 1, c], 0.0)
            line = tile8.T[:, row : row + 1]
            ref[c * width : (c + 1) * width, :] = jnp.broadcast_to(line, (width, LANES))
            from_left = rows_ref[first, c][row : row + 1, width - 1 : width]
            from_right = rows_ref[first + 2, c][row : row + 1, 0:1]
            corner.append(jnp.where(there & has_left, from_left, 0.0))
            corner.append(jnp.where(there & has_right, from_right, 0.0))
        corner = jnp.concatenate(corner + [jnp.zeros((4, 1), F32)], axis=0)
        ref[2 * width :, :] = jnp.broadcast_to(corner, (8, LANES))


GROUP = 8
STEP = 4
SIDE = 4


def weight_rows(data, cell, sub16, height):
    node_a = jnp.where(cell >= 0, cell >> 7, 2 * height)
    below, same, above = quad_weights(data)
    parts = [two_parts(w[0:1, :]) for w in (below, same, above)]

    def wide(v):
        return jnp.broadcast_to(v, (16, CAP))

    def wide16(v):
        return wide(v.astype(F32).astype(BF16))

    a_in, a_page = node_a & 15, node_a >> 4
    a_next = jnp.where(a_in == 15, a_page + 1, jnp.where(a_in == 0, a_page - 1, -9))
    in16, page16, next16 = wide16(a_in), wide16(a_page), wide16(a_next)
    is_below, is_same, is_above = sub16 == in16 - BF16(1), sub16 == in16, sub16 == in16 + BF16(1)
    wrap_up, wrap_down = sub16 == in16 - BF16(15), sub16 == in16 + BF16(15)
    none = jnp.zeros((16, CAP), BF16)
    near, far = [], []
    for h in range(2):
        low, mid, high = (wide(p[h]) for p in parts)
        near.append(jnp.where(is_below, low, jnp.where(is_same, mid, jnp.where(is_above, high, none))))
        far.append(jnp.where(wrap_up, high, jnp.where(wrap_down, low, none)))
    return near, far, page16, next16, none


def build_weights(data, cell, weight_ref, lanes, height):
    sub16 = lax.broadcasted_iota(I32, (16, CAP), 0).astype(F32).astype(BF16)
    near, far, page16, next16, none = weight_rows(data, cell, sub16, height)
    for c in range(height // 16):
        here_c, next_c = page16 == BF16(c), next16 == BF16(c)
        for h in range(2):
            rows = jnp.where(here_c, near[h], jnp.where(next_c, far[h], none))
            at = h * height + 16 * c
            weight_ref[at : at + 16, lanes] = rows


def mix(field_ref, weight_ref, height):
    weights = weight_ref[...]
    stacked = jnp.concatenate([weights, weights[0:height]], axis=0)
    return jnp.dot(field_ref[...], stacked, preferred_element_type=F32)


def pick_columns(data, cell, mixed_ref, up_ref, down_ref, lanes, height, width):
    sub8 = lax.broadcasted_iota(I32, (8, CAP), 0)
    node_b = cell & 127
    trio = quad_weights(data)

    def wide(v):
        return jnp.broadcast_to(v, (8, CAP))

    low, mid, high = (wide(w[1:2, :]) for w in trio)
    b_in, b_page = wide(node_b & 7), wide(node_b >> 3)
    b_next = jnp.where(b_in == 7, b_page + 1, jnp.where(b_in == 0, b_page - 1, -9))
    near = jnp.where(sub8 == b_in - 1, low, jnp.where(sub8 == b_in, mid, jnp.where(sub8 == b_in + 1, high, 0.0)))
    far = jnp.where(sub8 == b_in - 7, high, jnp.where(sub8 == b_in + 7, low, 0.0))
    first = cell < width
    edge = jnp.where(first, trio[0][0:1, :], jnp.where(cell >= (height - 1) * width, trio[2][0:1, :], 0.0))
    edge, first = wide(jnp.where(cell >= 0, edge, 0.0)), wide(cell) < width

    def rows_at(at):
        up = jnp.concatenate([up_ref[at : at + 8, :]] * 2, axis=1)
        down = jnp.concatenate([down_ref[at : at + 8, :]] * 2, axis=1)
        return mixed_ref[at : at + 8, lanes] + jnp.where(first, up, down) * edge

    picked = [[jnp.zeros((8, CAP), F32)] * 2 for _ in range(2)]
    for c in range(width // 8):
        here_c, next_c = b_page == c, b_next == c
        for k in range(2):
            block = rows_at(k * width + 8 * c)
            picked[k][0] = jnp.where(here_c, block, picked[k][0])
            picked[k][1] = jnp.where(next_c, block, picked[k][1])
    speed = []
    sides = rows_at(2 * width)
    for k in range(2):
        other = jnp.where(b_next == -1, wide(sides[2 * k : 2 * k + 1, :]), picked[k][1])
        other = jnp.where(b_next == width // 8, wide(sides[2 * k + 1 : 2 * k + 2, :]), other)
        speed.append(jnp.sum(picked[k][0] * near + other * far, axis=0, keepdims=True))
    shift = jnp.where(sub8 == 2, speed[0], jnp.where(sub8 == 3, speed[1], 0.0))
    return data + step_length * shift


def build_step(base, arrived_ref, cell_ref, weight_ref, height):
    for i in range(STEP):
        s = base + i
        here = pl.ds(pl.multiple_of(s * CAP, CAP), CAP)
        lanes = slice(i * CAP, (i + 1) * CAP)
        build_weights(arrived_ref[:, here], cell_ref[s], weight_ref, lanes, height)


def pick_step(base, arrived_ref, cell_ref, out_ref, mixed_ref, up_ref, down_ref, height, width):
    for i in range(STEP):
        s = base + i
        here = pl.ds(pl.multiple_of(s * CAP, CAP), CAP)
        lanes = slice(i * CAP, (i + 1) * CAP)
        out_ref[:, here] = pick_columns(
            arrived_ref[:, here], cell_ref[s], mixed_ref, up_ref, down_ref, lanes, height, width
        )


def wrapped(at, step, length):
    to = at + step
    return jnp.where(to >= length, to - length, to)


def rebin_kernel(
    sizes, part_in, key_in, a_in, b_in, vel_in, out_ref, cell_ref,
    part_ref, key_ref, a_ref, b_ref, vel_ref,
    pos_ref, acc_ref, sorted_ref, sorted_cell_ref, table_ref, table_smem,
    send_ref, send_cell_ref, turned_ref, rows_ref, cols_ref, field_ref, up_ref, down_ref, arrived_ref,
    weight0_ref, weight1_ref, mixed0_ref, mixed1_ref,
    load_sem, table_sem, send_sem, send_cell_sem, recv_sem, recv_cell_sem, halo_send, halo_recv,
):
    nx, ny, nz = sizes
    total = nx * ny * nz
    pairs = ((key_in, key_ref), (vel_in, vel_ref), (part_in, part_ref), (a_in, a_ref), (b_in, b_ref))
    loads = [pltpu.make_async_copy(src, dst, load_sem.at[k]) for k, (src, dst) in enumerate(pairs)]
    for load in loads:
        load.start()
    x, y, z = (lax.axis_index(a) for a in AXES)
    me = (x * ny + y) * nz + z
    tiles = ny * nz
    tile = y * nz + z
    height, width = vel_ref.shape[1], vel_ref.shape[2]
    outer, inner = y // SIDE, y % SIDE
    steps = [(0, 0), (0, 1), (1, 0), (0, 3), (3, 0), (1, 1), (3, 3), (1, 3), (3, 1), (0, 2), (2, 0), (1, 2), (2, 1), (3, 2), (2, 3), (2, 2)]
    ahead_x = [wrapped(x, d, nx) for d in range(nx)]
    ahead_y = [wrapped(outer, d, ny // SIDE) for d in range(ny // SIDE)]
    ahead_i = [wrapped(inner, d, SIDE) for d in range(SIDE)]
    ahead_z = [z, 1 - z]

    barrier = pltpu.get_barrier_semaphore()
    for a, b in steps:
        for i in range(SIDE):
            for c in range(nz):
                if (a, b, i, c) != (0, 0, 0, 0):
                    device = (ahead_x[a], ahead_y[b] * SIDE + ahead_i[i], ahead_z[c])
                    pl.semaphore_signal(barrier, inc=1, device_id=device, device_id_type=MESH)

    halos = []
    for i, dx in enumerate((1, nx - 1)):
        edge = vel_ref.at[:, pl.ds(height - 8 if dx == 1 else 0, 8), :]
        for j, dt in enumerate((1, 0, tiles - 1)):
            halos.append((edge, rows_ref.at[3 * i + j], ahead_x[dx], wrapped(tile, dt, tiles)))
    for i, dt in enumerate((1, tiles - 1)):
        edge = turned_ref.at[:, pl.ds(width - 8 if dt == 1 else 0, 8), :]
        halos.append((edge, cols_ref.at[i], x, wrapped(tile, dt, tiles)))
    halo_copies = [
        pltpu.make_async_remote_copy(
            src_ref=src, dst_ref=dst, send_sem=halo_send.at[k], recv_sem=halo_recv.at[k],
            device_id=(to_x, to_t // nz, to_t % nz), device_id_type=MESH,
        )
        for k, (src, dst, to_x, to_t) in enumerate(halos)
    ]

    def between():
        loads[1].wait()
        turned_ref[0] = vel_ref[0].T
        turned_ref[1] = vel_ref[1].T
        for load in loads[2:]:
            load.wait()

    loads[0].wait()
    sort_phase(
        part_ref, key_ref, a_ref, b_ref, pos_ref, acc_ref, sorted_ref, sorted_cell_ref,
        table_ref, table_smem, table_sem, total, between,
    )
    pl.semaphore_wait(barrier, total - 1)
    for c in halo_copies:
        c.start()

    mine = pl.ds(pl.multiple_of(me * CAP, CAP), CAP)

    def first_of(a, b):
        return (ahead_x[a] * (ny // SIDE) + ahead_y[b]) * GROUP

    def send_group(g):
        a, b = steps[g]
        for i in range(SIDE):
            for c in range(nz):
                there = first_of(a, b) + ahead_i[i] * nz + ahead_z[c]
                if (a, b, i, c) == (0, 0, 0, 0):
                    pltpu.make_async_copy(send_ref.at[there], arrived_ref.at[:, mine], recv_sem.at[g]).start()
                    pltpu.make_async_copy(send_cell_ref.at[there], cell_ref.at[me], recv_cell_sem.at[g]).start()
                    continue
                device = (ahead_x[a], ahead_y[b] * SIDE + ahead_i[i], ahead_z[c])
                pltpu.make_async_remote_copy(
                    src_ref=send_ref.at[there], dst_ref=arrived_ref.at[:, mine], send_sem=send_sem,
                    recv_sem=recv_sem.at[g], device_id=device, device_id_type=MESH,
                ).start()
                pltpu.make_async_remote_copy(
                    src_ref=send_cell_ref.at[there], dst_ref=cell_ref.at[me], send_sem=send_cell_sem,
                    recv_sem=recv_cell_sem.at[g], device_id=device, device_id_type=MESH,
                ).start()

    for g, (a, b) in enumerate(steps):
        base = first_of(a, b)

        def expand_one(i, carry, base=base):
            expand(base + i, sorted_ref, sorted_cell_ref, table_smem, send_ref, send_cell_ref)
            return carry

        lax.fori_loop(0, GROUP, expand_one, 0, unroll=True)
        if g > 0:
            send_group(g - 1)
    groups = len(steps)
    send_group(groups - 1)

    for c in halo_copies:
        c.wait()
    prepare_field(sizes, turned_ref, rows_ref, cols_ref, field_ref, up_ref, down_ref)

    def source_base(g):
        shift = jnp.int32(2) * g
        step_x = lax.shift_right_arithmetic(jnp.int32(-1369213168), shift) & 3
        step_y = lax.shift_right_arithmetic(jnp.int32(-1182141244), shift) & 3
        back_x = (x + nx - step_x) % nx
        back_y = (outer + ny // SIDE - step_y) % (ny // SIDE)
        return (back_x * (ny // SIDE) + back_y) * GROUP

    def arrive(g):
        blocks = arrived_ref.at[:, pl.ds(0, GROUP * CAP)]
        pltpu.make_async_copy(blocks, blocks, recv_sem.at[g]).wait()
        few = cell_ref.at[pl.ds(0, GROUP)]
        pltpu.make_async_copy(few, few, recv_cell_sem.at[g]).wait()

    build = lambda base, ref: build_step(base, arrived_ref, cell_ref, ref, height)
    pick = lambda base, ref: pick_step(
        base, arrived_ref, cell_ref, out_ref, ref, up_ref, down_ref, height, width
    )
    arrive(0)
    start = source_base(0)
    build(start, weight0_ref)
    mixed0_ref[...] = mix(field_ref, weight0_ref, height)
    build(start + STEP, weight1_ref)

    def one_group(g, before):
        arrive(g)
        base = source_base(g)
        mixed1_ref[...] = mix(field_ref, weight1_ref, height)
        pick(before, mixed0_ref)
        build(base, weight0_ref)
        mixed0_ref[...] = mix(field_ref, weight0_ref, height)
        pick(before + STEP, mixed1_ref)
        build(base + STEP, weight1_ref)
        return base

    last = lax.fori_loop(1, groups, one_group, start)
    mixed1_ref[...] = mix(field_ref, weight1_ref, height)
    pick(last, mixed0_ref)
    pick(last + STEP, mixed1_ref)
    some = send_ref.at[pl.ds(0, total - 1)]
    some_cell = send_cell_ref.at[pl.ds(0, total - 1)]
    pltpu.make_async_copy(some, some, send_sem).wait()
    pltpu.make_async_copy(some_cell, some_cell, send_cell_sem).wait()


def shards(sizes, particles, dest_key, cell_a, cell_b, velocity):
    owners = sizes[0] * sizes[1] * sizes[2]
    count = particles.shape[1]
    parts, height, width = velocity.shape
    vmem = pl.BlockSpec(memory_space=pltpu.VMEM)
    dma = pltpu.SemaphoreType.DMA
    groups = owners // GROUP
    binned, binned_cell = pl.pallas_call(
        functools.partial(rebin_kernel, sizes),
        out_shape=(
            pltpu.VMEM((8, owners * CAP), F32),
            pltpu.VMEM((owners, 1, CAP), I32),
        ),
        in_specs=[pl.BlockSpec(memory_space=pltpu.HBM)] * 5,
        out_specs=(vmem,) * 2,
        scratch_shapes=[
            pltpu.VMEM(particles.shape, F32),
            pltpu.VMEM((1, count), I32),
            pltpu.VMEM((1, count), I32),
            pltpu.VMEM((1, count), I32),
            pltpu.VMEM(velocity.shape, F32),
            pltpu.VMEM((1, count), I32),
            pltpu.VMEM((576, CAP), F32),
            pltpu.VMEM((67, 8, LANES), F32),
            pltpu.VMEM((67, 1, LANES), I32),
            pltpu.VMEM((16, LANES), I32),
            pltpu.SMEM((16, LANES), I32),
            pltpu.VMEM((owners, 8, CAP), F32),
            pltpu.VMEM((owners, 1, CAP), I32),
            pltpu.VMEM((parts, width, height), F32),
            pltpu.VMEM((6, parts, 8, width), F32),
            pltpu.VMEM((2, parts, 8, height), F32),
            pltpu.VMEM((2 * width + 8, 3 * height), BF16),
            pltpu.VMEM((2 * width + 8, LANES), F32),
            pltpu.VMEM((2 * width + 8, LANES), F32),
            pltpu.VMEM((8, owners * CAP), F32),
            pltpu.VMEM((2 * height, STEP * CAP), BF16),
            pltpu.VMEM((2 * height, STEP * CAP), BF16),
            pltpu.VMEM((2 * width + 8, STEP * CAP), F32),
            pltpu.VMEM((2 * width + 8, STEP * CAP), F32),
            dma((5,)), dma, dma, dma, dma((groups,)), dma((groups,)), dma((8,)), dma((8,)),
        ],
        compiler_params=pltpu.CompilerParams(collective_id=0, has_side_effects=True),
        name="rebin",
    )(particles, dest_key.reshape(1, -1), cell_a.reshape(1, -1), cell_b.reshape(1, -1), velocity)
    return binned, binned_cell.reshape(-1)


def solution(mesh):
    sizes = tuple(mesh.shape[a] for a in AXES)
    in_specs = (P(None, AXES), P(AXES), P(AXES), P(AXES), P(None, "gx", ("gy", "gz")))
    out_specs = (P(None, AXES), P(AXES))
    return jax.shard_map(
        functools.partial(shards, sizes), mesh=mesh, in_specs=in_specs, out_specs=out_specs, check_vma=False
    )
```
